32 devices in a mesh: groups: 2 (over x), cells: 16 (over z, y, core).
Axes of the slice: x: 2, y: 2, z: 4, core: 2. Of those that a mesh axis runs over, the one named last changes fastest.
Arguments:
- pair_act: bfloat16 [768, 384, 128], P(('groups', 'cells')), parts along dimension 0, may hold values from -6 to 6
- pair_mask: int32 [768, 384], P(('groups', 'cells')), parts along dimension 0, may hold values from 0 to 1, as said below
- chain_ids: int32 [768], P('groups'), parts along dimension 0, may hold values from 0 to 3, never falling along the last dimension, each value on 1 to 192 neighbouring positions
- proj_weight: bfloat16 [128, 256], replicated, may hold values from -0.5 to 0.5
- gate_weight: bfloat16 [128, 128], replicated, may hold values from -0.5 to 0.5
- chain_bias: float32 [2, 128], replicated, may hold values from -4 to 4
- out_weight: bfloat16 [64, 128], replicated, may hold values from -0.75 to 0.75
- out_grad: bfloat16 [768, 384, 128], P(('groups', 'cells')), parts along dimension 0, may hold values from -6 to 6
Outputs:
- pair_grad: bfloat16 [768, 384, 128], P(('groups', 'cells')), parts along dimension 0
- proj_weight_grad: float32 [256, 256], P('groups'), parts along dimension 0
- gate_weight_grad: float32 [256, 128], P('groups'), parts along dimension 0
- out_weight_grad: float32 [128, 128], P('groups'), parts along dimension 0
The draws below stay inside these ranges and needn't reach their ends.
There are 2 independent parts, one for each index of `groups`. The reference program is written for one: setup_inputs(seed, part) draws one part's arguments, and reference() takes and returns one part's arrays. A program takes and returns all parts, laid end to end along the dimension named above; an argument that names none is the same for every part. Nothing has to cross between parts.
Inputs may be any that keep to these rules, and one draw needn't show every extreme that they name: pair_mask[i, j] = valid[i] * valid[j] for a 0 or 1 validity of each residue.
All inputs are finite; a program needn't handle non-finite values.
Results may differ from the reference program's by a relative error of at most 0.012.
Values may be sent and summed in bfloat16 or wider, within the bound.
No kernel may reach another device: no remote copies, remote signals or barrier semaphores. Data moves between devices by JAX's collectives and lax.ppermute only.
A program may use at most 64 MiB of HBM per device.

```python
import math
import jax
import jax.numpy as jnp
import numpy as np
from jax import lax

C = 128
H = 64
N = 384
N_CELLS = 16


def draw_pair_mask(key, part):
    valid = (jax.random.randint(jax.random.fold_in(key, 11), (N,), 0, 8) < 7).astype(jnp.int32)
    return valid[:, None] * valid[None, :]


def level_of(own_key, extent, pieces, low, top_value):
    gain, own = 1.0, jax.random.fold_in(own_key, 6)
    for dim, blocks in pieces:
        steps = jnp.exp(jax.random.uniform(jax.random.fold_in(own, dim), (blocks,), jnp.float32, low / len(pieces), top_value / len(pieces)))
        gain = gain * jnp.repeat(steps, extent[dim] // blocks).reshape([-1 if axis == dim else 1 for axis in range(len(extent))])
    return gain


def length_profile(number_of, total, bound, slope):
    weights = [(1 << 20) // math.isqrt(rank ** slope) + 1 for rank in range(2, number_of + 1)]
    rest, given = total - bound - (number_of - 1), [1] * (number_of - 1)
    while rest > 0:
        movable = [i for i in range(number_of - 1) if given[i] < bound]
        whole, budget = sum([weights[i] for i in movable]), rest
        for i in movable:
            addition = min(bound - given[i], max(1, budget * weights[i] // whole), rest)
            given[i] = given[i] + addition
            rest = rest - addition
    return np.array([bound] + given)


def uneven(own_key, number_of, total, bound, skew):
    if number_of == 2:
        one = jax.random.randint(own_key, (), max(1, total - bound), min(bound, total - 1) + 1)
        return jnp.stack([one, total - one])
    sizes = jnp.asarray(length_profile(number_of, total, bound, skew), jnp.int32)
    twos = (number_of - 1) // 2
    donor, sink = sizes[1:1 + 2 * twos:2], sizes[2:2 + 2 * twos:2]
    slack = jnp.minimum(donor - 1, bound - sink)
    shifted = jax.random.randint(jax.random.fold_in(own_key, 1), (twos,), 0, 1 << 20) % (slack + 1)
    sizes = sizes.at[1:1 + 2 * twos:2].set(donor - shifted).at[2:2 + 2 * twos:2].set(sink + shifted)
    return sizes[jax.random.permutation(jax.random.fold_in(own_key, 2), number_of)]


def noise(stream_key, shape, spread, limit, cuts=(), kind=jnp.bfloat16):
    gain = level_of(stream_key, shape, cuts, -0.22, 0.18) if cuts else 1.0
    result = jax.random.normal(stream_key, shape, jnp.float32) * spread * gain
    return jnp.minimum(jnp.maximum(result, -limit), limit).astype(kind)


def setup_inputs(seed: int = 0, part: int = 0) -> dict:
    keys = jax.random.split(jax.random.key(seed), 9)
    part_keys = jax.random.split(jax.random.fold_in(keys[8], part), 9)
    pair_act = noise(part_keys[0], (N, N, C), 1.0, 6.0, ((0, 16),))
    pair_mask = draw_pair_mask(jax.random.fold_in(jax.random.fold_in(keys[8], part), 71), part)
    chain_ids = jnp.searchsorted(jnp.cumsum(uneven(part_keys[2], 4, N, N // 2, 0)), jnp.arange(N), side="right").astype(jnp.int32)
    proj_weight = noise(keys[3], (C, 4 * H), C ** -0.5, 0.5)
    gate_weight = noise(keys[4], (C, C), C ** -0.5, 0.5)
    chain_bias = noise(keys[5], (2, C), 1.0, 4.0, (), jnp.float32)
    out_weight = noise(keys[6], (H, C), H ** -0.5, 0.75)
    out_grad = noise(part_keys[7], (N, N, C), 1.0, 6.0, ((0, 16),))
    return {"pair_act": pair_act, "pair_mask": pair_mask, "chain_ids": chain_ids, "proj_weight": proj_weight, "gate_weight": gate_weight, "chain_bias": chain_bias, "out_weight": out_weight, "out_grad": out_grad}


EPS = 1e-05

def matmul(left, right):
    return jnp.dot(left.astype(jnp.float32), right.astype(jnp.float32), precision=lax.Precision.HIGHEST)

def normalize_last(values):
    center = values - lax.optimization_barrier(jnp.mean(values, axis=-1, keepdims=True))
    scale = lax.rsqrt(lax.optimization_barrier(jnp.mean(center * center, axis=-1, keepdims=True)) + EPS)
    return (center * scale, scale)

def norm_backward(grad, normed, scale):
    first = lax.optimization_barrier(jnp.mean(grad, axis=-1, keepdims=True))
    second = lax.optimization_barrier(jnp.mean(grad * normed, axis=-1, keepdims=True))
    return scale * (grad - first - normed * second)

def reference(pair_act, pair_mask, chain_ids, proj_weight, gate_weight, chain_bias, out_weight, out_grad):
    rows = N // N_CELLS
    count = rows * N
    starts = jnp.arange(N_CELLS, dtype=jnp.int32) * rows

    def front(start):
        block = lax.dynamic_slice_in_dim(pair_act, start, rows, 0).astype(jnp.float32).reshape(count, C)
        normed, scale = normalize_last(block)
        normed_low = normed.astype(jnp.bfloat16)
        projected = matmul(normed_low, proj_weight)
        keeper = lax.dynamic_slice_in_dim(pair_mask, start, rows, 0).astype(jnp.float32).reshape(count, 1)
        values = projected[:, :2 * H]
        sigma = jax.nn.sigmoid(projected[:, 2 * H:])
        return (normed, scale, normed_low, values, sigma, keeper)

    def make_factors(start):
        parts = front(start)
        return (parts[5] * parts[4] * parts[3]).astype(jnp.bfloat16)
    stacked = lax.map(make_factors, starts)
    channel_major = jnp.transpose(stacked.reshape(N, N, 2 * H), (2, 0, 1))

    def product(index):
        left_rows = channel_major[index]
        right_rows = channel_major[index + H]
        return matmul(left_rows, right_rows.T)
    triangle = lax.map(product, jnp.arange(H, dtype=jnp.int32))

    def middle(carry, start):
        normed, scale, normed_low, values, sigma, keeper = front(start)
        block = lax.dynamic_slice_in_dim(triangle, start, rows, 1).reshape(H, count).T
        tri_hat, tri_scale = normalize_last(block)
        tri_low = tri_hat.astype(jnp.bfloat16)
        outputs = matmul(tri_low, out_weight)
        own_chain = lax.dynamic_slice_in_dim(chain_ids, start, rows, 0)
        same_chain = (own_chain[:, None] == chain_ids[None, :]).reshape(count, 1)
        logits = matmul(normed_low, gate_weight)
        logits = logits + jnp.where(same_chain, chain_bias[0][None, :], chain_bias[1][None, :])
        gating = jax.nn.sigmoid(logits)
        upstream = lax.dynamic_slice_in_dim(out_grad, start, rows, 0).astype(jnp.float32).reshape(count, C)
        d_outputs = (upstream * gating).astype(jnp.bfloat16)
        d_logits = (upstream * outputs * gating * (1.0 - gating)).astype(jnp.bfloat16)
        out_acc = carry[0] + matmul(tri_low.T, d_outputs)
        gate_acc = carry[1] + matmul(normed_low.T, d_logits)
        d_hat = matmul(d_outputs, out_weight.T)
        d_tri = norm_backward(d_hat, tri_hat, tri_scale).astype(jnp.bfloat16)
        return ((out_acc, gate_acc), (d_tri.T.reshape(H, rows, N), d_logits))
    initial = (jnp.zeros((H, C), jnp.float32), jnp.zeros((C, C), jnp.float32))
    (out_acc, gate_acc), (tri_blocks, logit_blocks) = lax.scan(middle, initial, starts)
    tri_grad = jnp.transpose(tri_blocks, (1, 0, 2, 3)).reshape(H, N, N)

    def back_product(index):
        cotangent = tri_grad[index]
        left_rows = channel_major[index]
        right_rows = channel_major[index + H]
        d_left = matmul(cotangent, right_rows)
        d_right = matmul(cotangent.T, left_rows)
        return (d_left.astype(jnp.bfloat16), d_right.astype(jnp.bfloat16))
    left_grads, right_grads = lax.map(back_product, jnp.arange(H, dtype=jnp.int32))
    factor_grad = jnp.concatenate([left_grads, right_grads], axis=0)

    def finish(carry, inputs):
        start, d_logits = inputs
        normed, scale, normed_low, values, sigma, keeper = front(start)
        d_factor = lax.dynamic_slice_in_dim(factor_grad, start, rows, 1).reshape(2 * H, count).T.astype(jnp.float32)
        d_values = d_factor * keeper * sigma
        d_gates = d_factor * keeper * values * sigma * (1.0 - sigma)
        d_proj = jnp.concatenate([d_values, d_gates], axis=1).astype(jnp.bfloat16)
        proj_acc = carry + matmul(normed_low.T, d_proj)
        d_normed = matmul(d_proj, proj_weight.T)
        d_normed = d_normed + matmul(d_logits, gate_weight.T)
        d_block = norm_backward(d_normed, normed, scale)
        return (proj_acc, d_block.astype(jnp.bfloat16).reshape(rows, N, C))
    proj_acc, grad_blocks = lax.scan(finish, jnp.zeros((C, 4 * H), jnp.float32), (starts, logit_blocks))
    pair_grad = grad_blocks.reshape(N, N, C)
    factor = 1.0 / N
    return (pair_grad, proj_acc * factor, gate_acc * factor, out_acc * factor)
```

```python
import functools

import jax
import jax.numpy as jnp
from jax import lax
from jax.experimental import pallas as pl
from jax.experimental.pallas import tpu as pltpu
from jax.sharding import PartitionSpec as P

EPS = 1e-05
F32 = jnp.float32
BF16 = jnp.bfloat16
VMEM_LIMIT = 60 * 1024 * 1024

NN = (((1,), (0,)), ((), ()))
NT = (((1,), (1,)), ((), ()))
TN = (((0,), (0,)), ((), ()))


def dot(left, right, dims):
    return lax.dot_general(left, right, dims, preferred_element_type=F32)


def sigmoid(x):
    return 0.5 * jnp.tanh(0.5 * x) + 0.5


def layer_norm(x, axis):
    center = x - jnp.mean(x, axis=axis, keepdims=True)
    scale = lax.rsqrt(jnp.mean(center * center, axis=axis, keepdims=True) + EPS)
    return center * scale, scale


def norm_back(grad, normed, scale, axis):
    first = jnp.mean(grad, axis=axis, keepdims=True)
    second = jnp.mean(grad * normed, axis=axis, keepdims=True)
    return scale * (grad - first - normed * second)


def load_weights(me_ref, wt_ref, w_s, hpo):
    kinds, owners = wt_ref.shape[0], wt_ref.shape[1]
    rows = []
    for kind in range(kinds):
        for s in range(owners):
            rows.append(wt_ref[kind, me_ref[0] ^ s])
    w_s[...] = jnp.concatenate(rows, axis=0).astype(BF16)


def front_kernel(owners, hpo, me_ref, x_ref, mask_ref, wt_ref, *refs):
    outs, w_s = refs[: 2 * owners], refs[2 * owners]

    @pl.when(pl.program_id(0) == 0)
    def _():
        load_weights(me_ref, wt_ref, w_s, hpo)

    hidden2 = 2 * owners * hpo
    for r in range(x_ref.shape[0]):
        zhat, _ = layer_norm(x_ref[r].astype(F32), 1)
        projected = dot(w_s[...], zhat.astype(BF16), NT)
        keep = mask_ref[r : r + 1, :].astype(F32)
        factors = (keep * sigmoid(projected[hidden2:]) * projected[:hidden2]).astype(BF16)
        for s in range(2 * owners):
            outs[s][r] = factors[s * hpo : (s + 1) * hpo]


def gate_of(zlow, gw_ref, bias_ref, ids_ref, own):
    logits = dot(zlow, gw_ref[...], NN)
    same = ids_ref[...] == own
    return sigmoid(logits + jnp.where(same, bias_ref[0:1, :], bias_ref[1:2, :]))


def gate_kernel(rows_block, me_ref, own_ref, x_ref, up_ref, gw_ref, bias_ref, ids_ref, ow_ref, dout_ref, dhat_ref, w_s):
    step = pl.program_id(0)

    @pl.when(step == 0)
    def _():
        load_ow(me_ref, ow_ref, w_s)

    for r in range(rows_block):
        zhat, _ = layer_norm(x_ref[r].astype(F32), 1)
        gating = gate_of(zhat.astype(BF16), gw_ref, bias_ref, ids_ref, own_ref[step * rows_block + r])
        d_out = (up_ref[r].astype(F32) * gating).astype(BF16)
        dout_ref[r] = d_out
        dhat_ref[r] = dot(w_s[...], d_out, NT)


def load_ow(me_ref, ow_ref, w_s):
    owners = ow_ref.shape[0]
    w_s[...] = jnp.concatenate([ow_ref[me_ref[0] ^ s] for s in range(owners)], axis=0).astype(BF16)


def mid_kernel(owners, hpo, *refs):
    tri, dhat_ref, outs = refs[:owners], refs[owners], refs[owners + 1 :]
    for r in range(dhat_ref.shape[0]):
        triangle = jnp.concatenate([t[r].astype(F32) for t in tri], axis=0)
        tri_hat, scale = layer_norm(triangle, 0)
        d_tri = norm_back(dhat_ref[r], tri_hat, scale, 0).astype(BF16)
        for s in range(owners):
            outs[s][r] = d_tri[s * hpo : (s + 1) * hpo]


def logit_kernel(owners, hpo, rows_block, me_ref, own_ref, x_ref, up_ref, dout_ref, gw_ref, bias_ref, ids_ref, ow_ref, *refs):
    tri = refs[:owners]
    dlog_ref, gate_ref, out_ref, w_s, gacc, oacc = refs[owners:]
    step = pl.program_id(0)

    @pl.when(step == 0)
    def _():
        load_ow(me_ref, ow_ref, w_s)
        gacc[...] = jnp.zeros_like(gacc)
        oacc[...] = jnp.zeros_like(oacc)

    for r in range(rows_block):
        zhat, _ = layer_norm(x_ref[r].astype(F32), 1)
        zlow = zhat.astype(BF16)
        gating = gate_of(zlow, gw_ref, bias_ref, ids_ref, own_ref[step * rows_block + r])
        triangle = jnp.concatenate([t[r].astype(F32) for t in tri], axis=0)
        tri_low = layer_norm(triangle, 0)[0].astype(BF16)
        outputs = dot(tri_low, w_s[...], TN)
        d_log = (up_ref[r].astype(F32) * outputs * gating * (1.0 - gating)).astype(BF16)
        dlog_ref[r] = d_log
        oacc[...] += dot(tri_low, dout_ref[r], NN)
        gacc[...] += dot(zlow, d_log, TN)

    @pl.when(step == pl.num_programs(0) - 1)
    def _():
        gate_ref[...] = gacc[...]
        for s in range(owners):
            out_ref[me_ref[0] ^ s] = oacc[s * hpo : (s + 1) * hpo, :]


def finish_kernel(owners, hpo, me_ref, x_ref, mask_ref, wt_ref, gw_ref, dlog_ref, *refs):
    da, db, dc = refs[:owners], refs[owners : 2 * owners], refs[2 * owners : 3 * owners]
    pg_ref, proj_ref, w_s, acc = refs[3 * owners :]
    step = pl.program_id(0)

    @pl.when(step == 0)
    def _():
        load_weights(me_ref, wt_ref, w_s, hpo)
        acc[...] = jnp.zeros_like(acc)

    hidden2 = 2 * owners * hpo
    for r in range(x_ref.shape[0]):
        zhat, scale = layer_norm(x_ref[r].astype(F32), 1)
        zlow = zhat.astype(BF16)
        projected = dot(w_s[...], zlow, NT)
        values, sigma = projected[:hidden2], sigmoid(projected[hidden2:])
        keep = mask_ref[r : r + 1, :].astype(F32)
        d_fac = jnp.concatenate(
            [t[r].astype(F32) for t in da] + [t[r].astype(F32) + u[r].astype(F32) for t, u in zip(db, dc)], axis=0
        )
        d_values = d_fac * keep * sigma
        d_proj = jnp.concatenate([d_values, d_values * values * (1.0 - sigma)], axis=0).astype(BF16)
        acc[...] += dot(d_proj, zlow, NN)
        d_normed = dot(d_proj, w_s[...], TN) + dot(dlog_ref[r], gw_ref[...], NT)
        pg_ref[r] = norm_back(d_normed, zhat, scale, 1).astype(BF16)

    @pl.when(step == pl.num_programs(0) - 1)
    def _():
        for kind in range(4):
            for s in range(owners):
                start = (kind * owners + s) * hpo
                proj_ref[kind, me_ref[0] ^ s] = acc[start : start + hpo, :]


def shuffle_matrix(rows, hpo, back):
    n = rows * hpo
    to, frm = lax.broadcasted_iota(jnp.int32, (n, n), 0), lax.broadcasted_iota(jnp.int32, (n, n), 1)
    if back:
        to, frm = frm, to
    return jnp.where((to % rows == frm // hpo) & (to // rows == frm % hpo), 1.0, 0.0).astype(BF16)


def spread(p_ref, raw, dest, hpo, group):
    n = group * hpo
    for g in range(raw.shape[0] // n):
        moved = dot(p_ref[...], raw[g * n : (g + 1) * n, :], NN).astype(BF16)
        for h in range(hpo):
            dest[h, g * group : (g + 1) * group, :] = moved[h * group : (h + 1) * group]


def tri_kernel(owners, hpo, rows, group, me_ref, *refs):
    devices = 2 * owners
    a_in, b_in = refs[:owners], refs[owners : owners + devices]
    refs = refs[owners + devices :]
    tri_out, a_out, b_out = refs[:owners], refs[owners], refs[owners + 1]
    araw, braw, a_s, b_s, p_s, q_s, sem_a, sem_b, sem_o = refs[owners + 2 :]
    size = rows * hpo
    copies_a = [pltpu.make_async_copy(a_in[s], araw.at[pl.ds(s * size, size)], sem_a.at[s]) for s in range(owners)]
    copies_b = [
        pltpu.make_async_copy(b_in[s], braw.at[pl.ds(pl.multiple_of((me_ref[0] ^ s) * size, size), size)], sem_b.at[s])
        for s in range(devices)
    ]
    for copy in copies_a + copies_b:
        copy.start()
    p_s[...] = shuffle_matrix(group, hpo, False)
    q_s[...] = shuffle_matrix(rows, hpo, True)
    for copy in copies_a:
        copy.wait()
    spread(p_s, araw, a_s, hpo, group)
    out_a = pltpu.make_async_copy(a_s, a_out, sem_o.at[0])
    out_a.start()
    for copy in copies_b:
        copy.wait()
    spread(p_s, braw, b_s, hpo, group)
    out_b = pltpu.make_async_copy(b_s, b_out, sem_o.at[1])
    out_b.start()
    for s in range(owners):
        block = jnp.concatenate(
            [dot(a_s[h, s * rows : (s + 1) * rows, :], b_s[h], NT) for h in range(hpo)], axis=0
        ).astype(BF16)
        tri_out[s][...] = dot(q_s[...], block, NN).astype(BF16)
    out_a.wait()
    out_b.wait()


def back_kernel(owners, hpo, rows, group, me_ref, *refs):
    devices = 2 * owners
    d_in, a_in, b_in = refs[:owners], refs[owners], refs[owners + 1]
    refs = refs[owners + 2 :]
    da_out, db_out = refs[:owners], refs[owners : owners + devices]
    draw, d_s, db_s, p_s, q_s, q2_s, acc, sem_d, sem_o = refs[owners + devices :]
    size = rows * hpo
    copies = [pltpu.make_async_copy(d_in[s], draw.at[pl.ds(s * size, size)], sem_d.at[s]) for s in range(owners)]
    for copy in copies:
        copy.start()
    p_s[...] = shuffle_matrix(group, hpo, False)
    q_s[...] = shuffle_matrix(rows, hpo, True)
    q2_s[...] = shuffle_matrix(group, hpo, True)
    for copy in copies:
        copy.wait()
    spread(p_s, draw, d_s, hpo, group)
    for h in range(hpo):
        acc[h] = dot(d_s[h], a_in[h], TN).astype(BF16)
    n = group * hpo
    for g in range(acc.shape[1] // group):
        block = jnp.concatenate([acc[h, g * group : (g + 1) * group, :] for h in range(hpo)], axis=0)
        db_s[g * n : (g + 1) * n, :] = dot(q2_s[...], block, NN).astype(BF16)
    copies = [
        pltpu.make_async_copy(db_s.at[pl.ds(pl.multiple_of((me_ref[0] ^ s) * size, size), size)], db_out[s], sem_o.at[s])
        for s in range(devices)
    ]
    for copy in copies:
        copy.start()
    for s in range(owners):
        block = jnp.concatenate(
            [dot(d_s[h, s * rows : (s + 1) * rows, :], b_in[h], NN) for h in range(hpo)], axis=0
        ).astype(BF16)
        da_out[s][...] = dot(q_s[...], block, NN).astype(BF16)
    for copy in copies:
        copy.wait()


def smem():
    return pl.BlockSpec(memory_space=pltpu.SMEM)


def whole(array):
    return pl.BlockSpec(array.shape, lambda i: (0,) * array.ndim)


def by_rows(array, block):
    return pl.BlockSpec((block,) + array.shape[1:], lambda i: (i,) + (0,) * (array.ndim - 1))


def cost(flops, moved):
    return pl.CostEstimate(flops=flops, bytes_accessed=moved, transcendentals=0)


def params():
    return pltpu.CompilerParams(vmem_limit_bytes=VMEM_LIMIT)


def fast_local(pair_act, pair_mask, chain_ids, proj_weight, gate_weight, chain_bias, out_weight, out_grad):
    devices = lax.axis_size("cells")
    owners = devices // 2
    rows, length, width = pair_act.shape
    hidden = out_weight.shape[0]
    hpo = hidden // owners
    count = rows * length
    index = lax.axis_index("cells").astype(jnp.int32)
    me = jnp.reshape(index, (1,))
    slot = jnp.reshape(index % owners, (1,))
    step = 8
    grid = (rows // step,)
    wt = proj_weight.T.astype(F32).reshape(4, owners, hpo, width)
    ow = out_weight.astype(F32).reshape(owners, hpo, width)
    piece = jax.ShapeDtypeStruct((rows, hpo, length), BF16)
    flat = jax.ShapeDtypeStruct((rows * hpo, length), BF16)

    def send(array, s):
        return lax.ppermute(array, "cells", [(c, c ^ s) for c in range(devices)])

    factors = pl.pallas_call(
        functools.partial(front_kernel, owners, hpo),
        grid=grid,
        in_specs=[smem(), by_rows(pair_act, step), by_rows(pair_mask, step), whole(wt)],
        out_specs=[by_rows(piece, step)] * (2 * owners),
        out_shape=[piece] * (2 * owners),
        scratch_shapes=[pltpu.VMEM((4 * hidden, width), BF16)],
        compiler_params=params(),
        cost_estimate=cost(8 * count * width * hidden, 8 * count * width),
        name="front",
    )(slot, pair_act, pair_mask, wt)
    a_own, b_own = factors[:owners], factors[owners:]
    order = list(range(owners, devices)) + list(range(owners - 1, 0, -1))
    b_got = {0: b_own[0]}
    a_got = {0: a_own[0]}
    for s in order:
        b_got[s] = send(b_own[s % owners], s)
        if s < owners:
            a_got[s] = send(a_own[s], s)

    start = index * rows
    own_chain = lax.dynamic_slice_in_dim(chain_ids, start, rows, 0)
    ids = jnp.broadcast_to(chain_ids[:, None], (length, width))
    dense = jax.ShapeDtypeStruct((rows, length, width), BF16)
    dhat_shape = jax.ShapeDtypeStruct((rows, hidden, length), F32)
    d_out, d_hat = pl.pallas_call(
        functools.partial(gate_kernel, step),
        grid=grid,
        in_specs=[smem(), smem(), by_rows(pair_act, step), by_rows(out_grad, step), whole(gate_weight), whole(chain_bias), whole(ids), whole(ow)],
        out_specs=[by_rows(dense, step), by_rows(dhat_shape, step)],
        out_shape=[dense, dhat_shape],
        scratch_shapes=[pltpu.VMEM((hidden, width), BF16)],
        compiler_params=params(),
        cost_estimate=cost(4 * count * width * width, 12 * count * width),
        name="gate",
    )(slot, own_chain, pair_act, out_grad, gate_weight, chain_bias, ids, ow)

    group = 256 // hpo
    half = owners * rows
    any_spec = pl.BlockSpec(memory_space=pl.ANY)
    vmem_spec = pl.BlockSpec(memory_space=pltpu.VMEM)
    tri_results = pl.pallas_call(
        functools.partial(tri_kernel, owners, hpo, rows, group),
        in_specs=[smem()] + [any_spec] * (owners + devices),
        out_specs=[vmem_spec] * owners + [any_spec] * 2,
        out_shape=[flat] * owners
        + [jax.ShapeDtypeStruct((hpo, half, length), BF16), jax.ShapeDtypeStruct((hpo, length, length), BF16)],
        scratch_shapes=[
            pltpu.VMEM((half * hpo, length), BF16),
            pltpu.VMEM((length * hpo, length), BF16),
            pltpu.VMEM((hpo, half, length), BF16),
            pltpu.VMEM((hpo, length, length), BF16),
            pltpu.VMEM((group * hpo, group * hpo), BF16),
            pltpu.VMEM((rows * hpo, rows * hpo), BF16),
            pltpu.SemaphoreType.DMA((owners,)),
            pltpu.SemaphoreType.DMA((devices,)),
            pltpu.SemaphoreType.DMA((2,)),
        ],
        compiler_params=params(),
        cost_estimate=cost(2 * hpo * half * length * length, 0),
        name="triangle",
    )(me, *[a_got[s].reshape(flat.shape) for s in range(owners)], *[b_got[s].reshape(flat.shape) for s in range(devices)])
    tri_own, a_all, b_all = tri_results[:owners], tri_results[owners], tri_results[owners + 1]
    tri_got = {0: tri_own[0].reshape(piece.shape)}
    for s in range(owners - 1, 0, -1):
        tri_got[s] = send(tri_own[s].reshape(piece.shape), s)
    tri = [tri_got[s] for s in range(owners)]

    d_own = pl.pallas_call(
        functools.partial(mid_kernel, owners, hpo),
        grid=grid,
        in_specs=[by_rows(piece, step)] * owners + [by_rows(dhat_shape, step)],
        out_specs=[by_rows(piece, step)] * owners,
        out_shape=[piece] * owners,
        compiler_params=params(),
        cost_estimate=cost(20 * count * hidden, 8 * count * hidden),
        name="middle",
    )(*tri, d_hat)
    d_got = {0: d_own[0]}
    for s in range(owners - 1, 0, -1):
        d_got[s] = send(d_own[s], s)

    gate_shape = jax.ShapeDtypeStruct((width, width), F32)
    out_shape = jax.ShapeDtypeStruct((owners, hpo, width), F32)
    d_log, gate_term, out_term = pl.pallas_call(
        functools.partial(logit_kernel, owners, hpo, step),
        grid=grid,
        in_specs=[smem(), smem(), by_rows(pair_act, step), by_rows(out_grad, step), by_rows(dense, step), whole(gate_weight), whole(chain_bias), whole(ids), whole(ow)]
        + [by_rows(piece, step)] * owners,
        out_specs=[by_rows(dense, step), whole(gate_shape), whole(out_shape)],
        out_shape=[dense, gate_shape, out_shape],
        scratch_shapes=[pltpu.VMEM((hidden, width), BF16), pltpu.VMEM((width, width), F32), pltpu.VMEM((hidden, width), F32)],
        compiler_params=params(),
        cost_estimate=cost(8 * count * width * width, 10 * count * width),
        name="logits",
    )(slot, own_chain, pair_act, out_grad, d_out, gate_weight, chain_bias, ids, ow, *tri)

    back = pl.pallas_call(
        functools.partial(back_kernel, owners, hpo, rows, group),
        in_specs=[smem()] + [any_spec] * owners + [vmem_spec] * 2,
        out_specs=[vmem_spec] * owners + [any_spec] * devices,
        out_shape=[flat] * (owners + devices),
        scratch_shapes=[
            pltpu.VMEM((half * hpo, length), BF16),
            pltpu.VMEM((hpo, half, length), BF16),
            pltpu.VMEM((length * hpo, length), BF16),
            pltpu.VMEM((group * hpo, group * hpo), BF16),
            pltpu.VMEM((rows * hpo, rows * hpo), BF16),
            pltpu.VMEM((group * hpo, group * hpo), BF16),
            pltpu.VMEM((hpo, length, length), BF16),
            pltpu.SemaphoreType.DMA((owners,)),
            pltpu.SemaphoreType.DMA((devices,)),
        ],
        compiler_params=params(),
        cost_estimate=cost(4 * hpo * half * length * length, 0),
        name="back",
    )(me, *[d_got[s].reshape(flat.shape) for s in range(owners)], a_all, b_all)
    da_own, db_own = back[:owners], back[owners:]
    da_got = {0: da_own[0].reshape(piece.shape)}
    db_got = {0: db_own[0].reshape(piece.shape)}
    for s in order:
        db_got[s] = send(db_own[s].reshape(piece.shape), s)
        if s < owners:
            da_got[s] = send(da_own[s].reshape(piece.shape), s)

    def total(term):
        s = 1
        while s < devices:
            term = term + send(term, s)
            s *= 2
        return term

    small = total(jnp.concatenate([gate_term, out_term.reshape(hidden, width)], axis=0))

    proj_shape = jax.ShapeDtypeStruct((4, owners, hpo, width), F32)
    pair_grad, proj_term = pl.pallas_call(
        functools.partial(finish_kernel, owners, hpo),
        grid=grid,
        in_specs=[smem(), by_rows(pair_act, step), by_rows(pair_mask, step), whole(wt), whole(gate_weight), by_rows(dense, step)]
        + [by_rows(piece, step)] * (3 * owners),
        out_specs=[by_rows(dense, step), whole(proj_shape)],
        out_shape=[dense, proj_shape],
        scratch_shapes=[pltpu.VMEM((4 * hidden, width), BF16), pltpu.VMEM((4 * hidden, width), F32)],
        compiler_params=params(),
        cost_estimate=cost(24 * count * width * hidden, 12 * count * width),
        name="finish",
    )(
        slot, pair_act, pair_mask, wt, gate_weight, d_log,
        *[da_got[s] for s in range(owners)],
        *[db_got[s] for s in range(owners)],
        *[db_got[s + owners] for s in range(owners)],
    )
    proj_sum = total(proj_term.reshape(4 * hidden, width))
    factor = 1.0 / length
    return (pair_grad, proj_sum.T * factor, small[:width] * factor, small[width:] * factor)


def takes_fast(devices, pair_act, out_weight):
    rows, length, width = pair_act.shape
    hidden = out_weight.shape[0]
    owners = devices // 2
    return (
        devices & (devices - 1) == 0
        and 2 <= devices <= 16
        and rows % 8 == 0
        and hidden == 8 * owners
        and length % 128 == 0
        and width % 128 == 0
        and (owners * rows) % 32 == 0
    )


def normalize_axis(values, axis):
    center = values - jnp.mean(values, axis=axis, keepdims=True)
    scale = lax.rsqrt(jnp.mean(center * center, axis=axis, keepdims=True) + EPS)
    return (center * scale, scale)


def norm_backward(grad, normed, scale, axis):
    first = jnp.mean(grad, axis=axis, keepdims=True)
    second = jnp.mean(grad * normed, axis=axis, keepdims=True)
    return scale * (grad - first - normed * second)


def generic_local(
    pair_act, pair_mask, chain_ids, proj_weight, gate_weight, chain_bias, out_weight, out_grad
):
    devices = lax.axis_size("cells")
    rows_here = pair_act.shape[0]
    length = pair_act.shape[1]
    width = pair_act.shape[2]
    hidden = out_weight.shape[0]
    halfway = length // 2
    channel_pairs = devices // 2
    per_device = 2 * hidden // devices
    count = rows_here * length
    zfull = pair_act.astype(jnp.float32).reshape(count, width)
    zhat, zscale = normalize_axis(zfull, 1)
    normed = zhat.astype(jnp.bfloat16)
    projected = jnp.einsum("xc,cf->fx", normed, proj_weight, preferred_element_type=jnp.float32)
    keeper = pair_mask.astype(jnp.float32).reshape(1, count)
    values = projected[: 2 * hidden]
    sigma = jax.nn.sigmoid(projected[2 * hidden :])
    factors = (keeper * sigma * values).astype(jnp.bfloat16)
    outgoing = factors.reshape(2, channel_pairs, per_device, rows_here, 2, halfway)
    outgoing = jnp.transpose(outgoing, (1, 4, 0, 2, 3, 5)).reshape(
        devices, 2, per_device, rows_here, halfway
    )
    arrived = lax.all_to_all(outgoing, "cells", split_axis=0, concat_axis=3, tiled=True)
    left_half = arrived[0, 0]
    right_half = arrived[0, 1]
    partial_value = jnp.einsum(
        "cik,cjk->cij", left_half, right_half, preferred_element_type=jnp.float32
    )
    landed = lax.all_to_all(
        partial_value.reshape(per_device, devices, rows_here, length).astype(jnp.bfloat16),
        "cells",
        split_axis=1,
        concat_axis=0,
        tiled=True,
    ).astype(jnp.float32)
    landed = landed.reshape(channel_pairs, 2, per_device, rows_here, length)
    triangle = jnp.sum(landed, axis=1).reshape(hidden, count)
    tri_hat, tri_scale = normalize_axis(triangle, 0)
    tri_low = tri_hat.astype(jnp.bfloat16)
    outputs = jnp.einsum("hx,hc->xc", tri_low, out_weight, preferred_element_type=jnp.float32)
    start = lax.axis_index("cells") * rows_here
    own_chain = lax.dynamic_slice_in_dim(chain_ids, start, rows_here, 0)
    same_chain = (own_chain[:, None] == chain_ids[None, :]).reshape(count, 1)
    logits = jnp.dot(normed, gate_weight, preferred_element_type=jnp.float32)
    logits = logits + jnp.where(same_chain, chain_bias[0][None, :], chain_bias[1][None, :])
    gating = jax.nn.sigmoid(logits)
    upstream = out_grad.reshape(count, width).astype(jnp.float32)
    d_outputs = (upstream * gating).astype(jnp.bfloat16)
    d_logits = (upstream * outputs * gating * (1.0 - gating)).astype(jnp.bfloat16)
    out_term = jnp.einsum("hx,xc->hc", tri_low, d_outputs, preferred_element_type=jnp.float32)
    gate_term = jnp.einsum("xc,xd->cd", normed, d_logits, preferred_element_type=jnp.float32)
    d_hat = jnp.einsum("xc,hc->hx", d_outputs, out_weight, preferred_element_type=jnp.float32)
    d_tri = norm_backward(d_hat, tri_hat, tri_scale, 0).astype(jnp.bfloat16)
    doubled = jnp.broadcast_to(
        d_tri.reshape(channel_pairs, 1, per_device, rows_here, length),
        (channel_pairs, 2, per_device, rows_here, length),
    )
    whole = lax.all_to_all(
        doubled.reshape(devices, per_device, rows_here, length),
        "cells",
        split_axis=0,
        concat_axis=2,
        tiled=True,
    )[0]
    d_left = jnp.einsum("cij,cjk->cik", whole, right_half, preferred_element_type=jnp.float32)
    d_right = jnp.einsum("cij,cik->cjk", whole, left_half, preferred_element_type=jnp.float32)
    d_pair = jnp.stack([d_left, d_right]).astype(jnp.bfloat16)
    returned = lax.all_to_all(
        d_pair.reshape(2, per_device, devices, rows_here, halfway),
        "cells",
        split_axis=2,
        concat_axis=2,
        tiled=True,
    )
    returned = returned.reshape(2, per_device, channel_pairs, 2, rows_here, halfway)
    d_factors = (
        jnp.transpose(returned, (0, 2, 1, 4, 3, 5)).reshape(2 * hidden, count).astype(jnp.float32)
    )
    d_values = d_factors * keeper * sigma
    d_gates = d_factors * keeper * values * sigma * (1.0 - sigma)
    d_proj = jnp.concatenate([d_values, d_gates], axis=0).astype(jnp.bfloat16)
    proj_term = jnp.einsum("xc,fx->cf", normed, d_proj, preferred_element_type=jnp.float32)
    d_normed = jnp.einsum("fx,cf->xc", d_proj, proj_weight, preferred_element_type=jnp.float32)
    d_normed = d_normed + jnp.einsum(
        "xd,cd->xc", d_logits, gate_weight, preferred_element_type=jnp.float32
    )
    pair_grad = (
        norm_backward(d_normed, zhat, zscale, 1)
        .astype(jnp.bfloat16)
        .reshape(rows_here, length, width)
    )
    proj_sum, gate_sum, out_sum = lax.psum((proj_term, gate_term, out_term), "cells")
    factor = 1.0 / length
    return (pair_grad, proj_sum * factor, gate_sum * factor, out_sum * factor)


def local(*arrays):
    if takes_fast(lax.axis_size("cells"), arrays[0], arrays[6]):
        return fast_local(*arrays)
    return generic_local(*arrays)


def solution(mesh):
    placed = (
        P(("groups", "cells"), None, None),
        P(("groups", "cells"), None),
        P("groups"),
        P(),
        P(),
        P(),
        P(),
        P(("groups", "cells"), None, None),
    )
    return jax.shard_map(
        local,
        mesh=mesh,
        in_specs=placed,
        out_specs=(
            P(("groups", "cells"), None, None),
            P("groups", None),
            P("groups", None),
            P("groups", None),
        ),
        check_vma=False,
    )
```

```python
import functools

import jax
import jax.numpy as jnp
from jax import lax
from jax.experimental import pallas as pl
from jax.experimental.pallas import tpu as pltpu
from jax.sharding import PartitionSpec as P


EPS = 1e-05
F32 = jnp.float32
BF16 = jnp.bfloat16
VMEM_LIMIT = 60 * 1024 * 1024

NN = (((1,), (0,)), ((), ()))
NT = (((1,), (1,)), ((), ()))
TN = (((0,), (0,)), ((), ()))


def dot(left, right, dims):
    return lax.dot_general(left, right, dims, preferred_element_type=F32)


def sigmoid(x):
    return 0.5 * jnp.tanh(0.5 * x) + 0.5


def layer_norm(x, axis):
    center = x - jnp.mean(x, axis=axis, keepdims=True)
    scale = lax.rsqrt(jnp.mean(center * center, axis=axis, keepdims=True) + EPS)
    return center * scale, scale


def lane_mean(*terms):
    both = jnp.concatenate(terms, axis=1)
    return dot(both, jnp.full((both.shape[1], terms[0].shape[1]), 1.0 / terms[0].shape[1], BF16), NN)


def row_norm(low):
    return layer_norm(low.astype(F32), 1)


def row_norm_back(grad, normed, scale):
    first = lane_mean(grad.astype(BF16))
    second = lane_mean((grad * normed).astype(BF16))
    return scale * (grad - first - normed * second)


def norm_back(grad, normed, scale, axis):
    first = jnp.mean(grad, axis=axis, keepdims=True)
    second = jnp.mean(grad * normed, axis=axis, keepdims=True)
    return scale * (grad - first - normed * second)


def load_weights(me_ref, proj_ref, t_s, w_s, kinds):
    t_s[...] = proj_ref[...].astype(F32).T.reshape(t_s.shape)
    owners = t_s.shape[0] // 4
    rows = []
    for kind in kinds:
        for s in range(owners):
            block = t_s[kind * owners + (me_ref[0] ^ s)]
            rows.append(block if kind < 2 else 0.5 * block)
    w_s[...] = jnp.concatenate(rows, axis=0).astype(BF16)


def front_kernel(owners, hpo, me_ref, x_ref, mask_ref, wt_ref, *refs):
    outs, t_s, w_s = refs[: 2 * owners], refs[2 * owners], refs[2 * owners + 1]

    @pl.when(pl.program_id(0) == 0)
    def _():
        load_weights(me_ref, wt_ref, t_s, w_s, (0, 1, 2, 3))

    hidden2 = 2 * owners * hpo
    for r in range(x_ref.shape[0]):
        zhat, _ = row_norm(x_ref[r])
        projected = dot(w_s[...], zhat.astype(BF16), NT)
        keep = 0.5 * mask_ref[r : r + 1, :].astype(F32)
        factors = ((keep * jnp.tanh(projected[hidden2:]) + keep) * projected[:hidden2]).astype(BF16)
        for s in range(2 * owners):
            outs[s][r] = factors[s * hpo : (s + 1) * hpo]


def gate_of(zlow, gw_ref, bias_ref, ids_ref, own):
    logits = dot(zlow, gw_ref[...], NN)
    same = ids_ref[...] == own
    return sigmoid(logits + jnp.where(same, bias_ref[0:1, :], bias_ref[1:2, :]))


def gate_kernel(rows_block, me_ref, own_ref, x_ref, up_ref, gw_ref, bias_ref, ids_ref, ow_ref, dout_ref, dhat_ref, w_s):
    step = pl.program_id(0)

    @pl.when(step == 0)
    def _():
        load_ow(me_ref, ow_ref, w_s)

    for r in range(rows_block):
        zhat, _ = row_norm(x_ref[r])
        gating = gate_of(zhat.astype(BF16), gw_ref, bias_ref, ids_ref, own_ref[step * rows_block + r])
        d_out = (up_ref[r].astype(F32) * gating).astype(BF16)
        dout_ref[r] = d_out
        dhat_ref[r] = dot(w_s[...], d_out, NT)


def load_ow(me_ref, ow_ref, w_s):
    owners = ow_ref.shape[0]
    w_s[...] = jnp.concatenate([ow_ref[me_ref[0] ^ s] for s in range(owners)], axis=0).astype(BF16)


def mid_kernel(owners, hpo, *refs):
    tri, dhat_ref, outs = refs[:owners], refs[owners], refs[owners + 1 :]
    for r in range(dhat_ref.shape[0]):
        triangle = jnp.concatenate([t[r].astype(F32) for t in tri], axis=0)
        tri_hat, scale = layer_norm(triangle, 0)
        d_tri = norm_back(dhat_ref[r], tri_hat, scale, 0).astype(BF16)
        for s in range(owners):
            outs[s][r] = d_tri[s * hpo : (s + 1) * hpo]


def logit_kernel(owners, hpo, rows_block, me_ref, own_ref, x_ref, up_ref, dout_ref, gw_ref, bias_ref, ids_ref, ow_ref, *refs):
    tri = refs[:owners]
    dlog_ref, gate_ref, out_ref, w_s, gacc, oacc = refs[owners:]
    step = pl.program_id(0)

    @pl.when(step == 0)
    def _():
        load_ow(me_ref, ow_ref, w_s)
        gacc[...] = jnp.zeros_like(gacc)
        oacc[...] = jnp.zeros_like(oacc)

    for r in range(rows_block):
        zhat, _ = row_norm(x_ref[r])
        zlow = zhat.astype(BF16)
        gating = gate_of(zlow, gw_ref, bias_ref, ids_ref, own_ref[step * rows_block + r])
        triangle = jnp.concatenate([t[r].astype(F32) for t in tri], axis=0)
        tri_low = layer_norm(triangle, 0)[0].astype(BF16)
        outputs = dot(tri_low, w_s[...], TN)
        d_log = (up_ref[r].astype(F32) * outputs * gating * (1.0 - gating)).astype(BF16)
        dlog_ref[r] = d_log
        oacc[...] += dot(tri_low, dout_ref[r], NN)
        gacc[...] += dot(zlow, d_log, TN)

    @pl.when(step == pl.num_programs(0) - 1)
    def _():
        gate_ref[...] = gacc[...]
        for s in range(owners):
            out_ref[me_ref[0] ^ s] = oacc[s * hpo : (s + 1) * hpo, :]


def part_grad(hidden, mask_row, w_s, zlow, d_fac):
    projected = dot(w_s[...], zlow, NT)
    values, bent = projected[:hidden], jnp.tanh(projected[hidden:])
    keep = 0.5 * mask_row.astype(F32)
    d_values = d_fac * (keep * bent + keep)
    return jnp.concatenate([d_values, d_values * (values - values * bent)], axis=0).astype(BF16)


def store_proj(me_ref, acc, proj_ref, owners, hpo):
    for kind in range(2):
        for s in range(owners):
            start = (kind * owners + s) * hpo
            block = acc[start : start + hpo, :]
            proj_ref[kind, me_ref[0] ^ s] = 0.5 * block if kind else block


def left_kernel(owners, hpo, me_ref, x_ref, mask_ref, wt_ref, gw_ref, dlog_ref, *refs):
    da = refs[:owners]
    part_ref, zlow_ref, proj_ref, t_s, w_s, acc = refs[owners:]
    step = pl.program_id(0)

    @pl.when(step == 0)
    def _():
        load_weights(me_ref, wt_ref, t_s, w_s, (0, 2))
        acc[...] = jnp.zeros_like(acc)

    for r in range(x_ref.shape[0]):
        zlow = row_norm(x_ref[r])[0].astype(BF16)
        zlow_ref[r] = zlow
        d_fac = jnp.concatenate([t[r].astype(F32) for t in da], axis=0)
        d_proj = part_grad(owners * hpo, mask_ref[r : r + 1, :], w_s, zlow, d_fac)
        acc[...] += dot(d_proj, zlow, NN)
        part_ref[r] = dot(d_proj, w_s[...], TN) + dot(dlog_ref[r], gw_ref[...], NT)

    @pl.when(step == pl.num_programs(0) - 1)
    def _():
        store_proj(me_ref, acc, proj_ref, owners, hpo)


def right_kernel(owners, hpo, me_ref, zlow_ref, mask_ref, wt_ref, _early, *refs):
    db, dc = refs[:owners], refs[owners : 2 * owners]
    dproj_ref, proj_ref, t_s, w_s, acc = refs[2 * owners :]
    step = pl.program_id(0)

    @pl.when(step == 0)
    def _():
        load_weights(me_ref, wt_ref, t_s, w_s, (1, 3))
        acc[...] = jnp.zeros_like(acc)

    for r in range(zlow_ref.shape[0]):
        zlow = zlow_ref[r]
        d_fac = jnp.concatenate([t[r].astype(F32) + u[r].astype(F32) for t, u in zip(db, dc)], axis=0)
        d_proj = part_grad(owners * hpo, mask_ref[r : r + 1, :], w_s, zlow, d_fac)
        dproj_ref[r] = d_proj
        acc[...] += dot(d_proj, zlow, NN)

    @pl.when(step == pl.num_programs(0) - 1)
    def _():
        store_proj(me_ref, acc, proj_ref, owners, hpo)


def finish_kernel(me_ref, x_ref, wt_ref, part_ref, dproj_ref, pg_ref, t_s, w_s):
    @pl.when(pl.program_id(0) == 0)
    def _():
        load_weights(me_ref, wt_ref, t_s, w_s, (1, 3))

    for r in range(x_ref.shape[0]):
        zhat, scale = row_norm(x_ref[r])
        d_normed = part_ref[r] + dot(dproj_ref[r], w_s[...], TN)
        pg_ref[r] = row_norm_back(d_normed, zhat, scale).astype(BF16)


def shuffle_matrix(rows, hpo):
    n = rows * hpo
    to, frm = lax.broadcasted_iota(jnp.int32, (n, n), 0), lax.broadcasted_iota(jnp.int32, (n, n), 1)
    return jnp.where((to % rows == frm // hpo) & (to // rows == frm % hpo), 1.0, 0.0).astype(BF16)


def spread(p_ref, raw, dest, hpo, group):
    n = group * hpo
    for g in range(raw.shape[0] // n):
        moved = dot(p_ref[...], raw[g * n : (g + 1) * n, :], NN).astype(BF16)
        for h in range(hpo):
            dest[h, g * group : (g + 1) * group, :] = moved[h * group : (h + 1) * group]


def unspread(sums, outs, rows):
    for s in range(len(outs)):
        block = sums[s * rows : (s + 1) * rows]
        outs[s][...] = block.reshape(outs[s].shape).astype(BF16)


def tri_kernel(owners, hpo, rows, group, me_ref, *refs):
    devices = 2 * owners
    a_in, b_in = refs[:owners], refs[owners : owners + devices]
    refs = refs[owners + devices :]
    tri_out, a_out, b_out = refs[:owners], refs[owners], refs[owners + 1]
    araw, braw, a_s, b_s, t_s, p_s, sem_a, sem_b, sem_o = refs[owners + 2 :]
    size = rows * hpo
    copies_a = [pltpu.make_async_copy(a_in[s], araw.at[pl.ds(s * size, size)], sem_a.at[s]) for s in range(owners)]
    copies_b = [
        pltpu.make_async_copy(b_in[s], braw.at[pl.ds(pl.multiple_of((me_ref[0] ^ s) * size, size), size)], sem_b.at[s])
        for s in range(devices)
    ]
    for copy in copies_a + copies_b:
        copy.start()
    p_s[...] = shuffle_matrix(group, hpo)
    for copy in copies_a:
        copy.wait()
    spread(p_s, araw, a_s, hpo, group)
    out_a = pltpu.make_async_copy(a_s, a_out, sem_o.at[0])
    out_a.start()
    for copy in copies_b:
        copy.wait()
    spread(p_s, braw, b_s, hpo, group)
    out_b = pltpu.make_async_copy(b_s, b_out, sem_o.at[1])
    out_b.start()
    for h in range(hpo):
        t_s[:, h, :] = dot(a_s[h], b_s[h], NT)
    unspread(t_s, tri_out, rows)
    out_a.wait()
    out_b.wait()


def back_kernel(owners, hpo, rows, group, me_ref, *refs):
    devices = 2 * owners
    d_in, a_in, b_in = refs[:owners], refs[owners], refs[owners + 1]
    refs = refs[owners + 2 :]
    da_out, db_out = refs[:owners], refs[owners : owners + devices]
    draw, d_s, db_s, t_s, p_s, acc, sem_d, sem_o = refs[owners + devices :]
    size = rows * hpo
    copies = [pltpu.make_async_copy(d_in[s], draw.at[pl.ds(s * size, size)], sem_d.at[s]) for s in range(owners)]
    for copy in copies:
        copy.start()
    p_s[...] = shuffle_matrix(group, hpo)
    for copy in copies:
        copy.wait()
    spread(p_s, draw, d_s, hpo, group)
    for h in range(hpo):
        acc[:, h, :] = dot(d_s[h], a_in[h], TN)
    for s in range(devices):
        db_s[s * size : (s + 1) * size, :] = acc[s * rows : (s + 1) * rows].reshape(size, acc.shape[2]).astype(BF16)
    copies = [
        pltpu.make_async_copy(db_s.at[pl.ds(pl.multiple_of((me_ref[0] ^ s) * size, size), size)], db_out[s], sem_o.at[s])
        for s in range(devices)
    ]
    for copy in copies:
        copy.start()
    for h in range(hpo):
        t_s[:, h, :] = dot(d_s[h], b_in[h], NN)
    unspread(t_s, da_out, rows)
    for copy in copies:
        copy.wait()


def smem():
    return pl.BlockSpec(memory_space=pltpu.SMEM)


def whole(array):
    return pl.BlockSpec(array.shape, lambda i: (0,) * array.ndim)


def by_rows(array, block):
    return pl.BlockSpec((block,) + array.shape[1:], lambda i: (i,) + (0,) * (array.ndim - 1))


def cost(flops, moved):
    return pl.CostEstimate(flops=flops, bytes_accessed=moved, transcendentals=0)


def params():
    return pltpu.CompilerParams(vmem_limit_bytes=VMEM_LIMIT)


def fast_local(pair_act, pair_mask, chain_ids, proj_weight, gate_weight, chain_bias, out_weight, out_grad):
    devices = lax.axis_size("cells")
    owners = devices // 2
    rows, length, width = pair_act.shape
    hidden = out_weight.shape[0]
    hpo = hidden // owners
    count = rows * length
    index = lax.axis_index("cells").astype(jnp.int32)
    me = jnp.reshape(index, (1,))
    slot = jnp.reshape(index % owners, (1,))
    step = 8
    grid = (rows // step,)
    ow = out_weight.astype(F32).reshape(owners, hpo, width)
    turned = pltpu.VMEM((4 * owners, hpo, width), F32)
    piece = jax.ShapeDtypeStruct((rows, hpo, length), BF16)
    flat = jax.ShapeDtypeStruct((rows * hpo, length), BF16)

    def send(array, s):
        return lax.ppermute(array, "cells", [(c, c ^ s) for c in range(devices)])

    factors = pl.pallas_call(
        functools.partial(front_kernel, owners, hpo),
        grid=grid,
        in_specs=[smem(), by_rows(pair_act, step), by_rows(pair_mask, step), whole(proj_weight)],
        out_specs=[by_rows(piece, step)] * (2 * owners),
        out_shape=[piece] * (2 * owners),
        scratch_shapes=[turned, pltpu.VMEM((4 * hidden, width), BF16)],
        compiler_params=params(),
        cost_estimate=cost(8 * count * width * hidden, 8 * count * width),
        name="front",
    )(slot, pair_act, pair_mask, proj_weight)
    a_own, b_own = factors[:owners], factors[owners:]
    order = list(range(owners, devices)) + list(range(owners - 1, 0, -1))
    b_got = {0: b_own[0]}
    a_got = {0: a_own[0]}
    for s in order:
        b_got[s] = send(b_own[s % owners], s)
        if s < owners:
            a_got[s] = send(a_own[s], s)

    start = index * rows
    own_chain = lax.dynamic_slice_in_dim(chain_ids, start, rows, 0)
    ids = jnp.broadcast_to(chain_ids[:, None], (length, width))
    dense = jax.ShapeDtypeStruct((rows, length, width), BF16)
    dhat_shape = jax.ShapeDtypeStruct((rows, hidden, length), F32)
    d_out, d_hat = pl.pallas_call(
        functools.partial(gate_kernel, step),
        grid=grid,
        in_specs=[smem(), smem(), by_rows(pair_act, step), by_rows(out_grad, step), whole(gate_weight), whole(chain_bias), whole(ids), whole(ow)],
        out_specs=[by_rows(dense, step), by_rows(dhat_shape, step)],
        out_shape=[dense, dhat_shape],
        scratch_shapes=[pltpu.VMEM((hidden, width), BF16)],
        compiler_params=params(),
        cost_estimate=cost(4 * count * width * width, 12 * count * width),
        name="gate",
    )(slot, own_chain, pair_act, out_grad, gate_weight, chain_bias, ids, ow)

    group = 256 // hpo
    half = owners * rows
    any_spec = pl.BlockSpec(memory_space=pl.ANY)
    vmem_spec = pl.BlockSpec(memory_space=pltpu.VMEM)
    tri_results = pl.pallas_call(
        functools.partial(tri_kernel, owners, hpo, rows, group),
        in_specs=[smem()] + [any_spec] * (owners + devices),
        out_specs=[vmem_spec] * owners + [any_spec] * 2,
        out_shape=[flat] * owners
        + [jax.ShapeDtypeStruct((hpo, half, length), BF16), jax.ShapeDtypeStruct((hpo, length, length), BF16)],
        scratch_shapes=[
            pltpu.VMEM((half * hpo, length), BF16),
            pltpu.VMEM((length * hpo, length), BF16),
            pltpu.VMEM((hpo, half, length), BF16),
            pltpu.VMEM((hpo, length, length), BF16),
            pltpu.VMEM((half, hpo, length), F32),
            pltpu.VMEM((group * hpo, group * hpo), BF16),
            pltpu.SemaphoreType.DMA((owners,)),
            pltpu.SemaphoreType.DMA((devices,)),
            pltpu.SemaphoreType.DMA((2,)),
        ],
        compiler_params=params(),
        cost_estimate=cost(2 * hpo * half * length * length, 0),
        name="triangle",
    )(me, *[a_got[s].reshape(flat.shape) for s in range(owners)], *[b_got[s].reshape(flat.shape) for s in range(devices)])
    tri_own, a_all, b_all = tri_results[:owners], tri_results[owners], tri_results[owners + 1]
    tri_got = {0: tri_own[0].reshape(piece.shape)}
    for s in range(owners - 1, 0, -1):
        tri_got[s] = send(tri_own[s].reshape(piece.shape), s)
    tri = [tri_got[s] for s in range(owners)]

    d_own = pl.pallas_call(
        functools.partial(mid_kernel, owners, hpo),
        grid=grid,
        in_specs=[by_rows(piece, step)] * owners + [by_rows(dhat_shape, step)],
        out_specs=[by_rows(piece, step)] * owners,
        out_shape=[piece] * owners,
        compiler_params=params(),
        cost_estimate=cost(20 * count * hidden, 8 * count * hidden),
        name="middle",
    )(*tri, d_hat)
    d_got = {0: d_own[0]}
    for s in range(owners - 1, 0, -1):
        d_got[s] = send(d_own[s], s)

    gate_shape = jax.ShapeDtypeStruct((width, width), F32)
    out_shape = jax.ShapeDtypeStruct((owners, hpo, width), F32)
    d_log, gate_term, out_term = pl.pallas_call(
        functools.partial(logit_kernel, owners, hpo, step),
        grid=grid,
        in_specs=[smem(), smem(), by_rows(pair_act, step), by_rows(out_grad, step), by_rows(dense, step), whole(gate_weight), whole(chain_bias), whole(ids), whole(ow)]
        + [by_rows(piece, step)] * owners,
        out_specs=[by_rows(dense, step), whole(gate_shape), whole(out_shape)],
        out_shape=[dense, gate_shape, out_shape],
        scratch_shapes=[pltpu.VMEM((hidden, width), BF16), pltpu.VMEM((width, width), F32), pltpu.VMEM((hidden, width), F32)],
        compiler_params=params(),
        cost_estimate=cost(8 * count * width * width, 10 * count * width),
        name="logits",
    )(slot, own_chain, pair_act, out_grad, d_out, gate_weight, chain_bias, ids, ow, *tri)

    back = pl.pallas_call(
        functools.partial(back_kernel, owners, hpo, rows, group),
        in_specs=[smem()] + [any_spec] * owners + [vmem_spec] * 2,
        out_specs=[vmem_spec] * owners + [any_spec] * devices,
        out_shape=[flat] * (owners + devices),
        scratch_shapes=[
            pltpu.VMEM((half * hpo, length), BF16),
            pltpu.VMEM((hpo, half, length), BF16),
            pltpu.VMEM((length * hpo, length), BF16),
            pltpu.VMEM((half, hpo, length), F32),
            pltpu.VMEM((group * hpo, group * hpo), BF16),
            pltpu.VMEM((length, hpo, length), F32),
            pltpu.SemaphoreType.DMA((owners,)),
            pltpu.SemaphoreType.DMA((devices,)),
        ],
        compiler_params=params(),
        cost_estimate=cost(4 * hpo * half * length * length, 0),
        name="back",
    )(me, *[d_got[s].reshape(flat.shape) for s in range(owners)], a_all, b_all)
    da_own, db_own = back[:owners], back[owners:]
    da_got = {0: da_own[0].reshape(piece.shape)}
    db_got = {0: db_own[0].reshape(piece.shape)}
    for s in range(owners - 1, 0, -1):
        da_got[s] = send(da_own[s].reshape(piece.shape), s)
    for s in order:
        db_got[s] = send(db_own[s].reshape(piece.shape), s)

    low = index % 2 == 0

    def over_chip(term):
        n = term.shape[0] // 2
        first, second = term[:n], term[n:]
        mine = jnp.where(low, first, second) + send(jnp.where(low, second, first), 1)
        return mine + send(mine, 2)

    def over_rest(term):
        return term + sum(send(term, s) for s in range(4, devices, 4))

    proj_shape = jax.ShapeDtypeStruct((2, owners, hpo, width), F32)
    part_shape = jax.ShapeDtypeStruct((rows, length, width), F32)
    dproj_shape = jax.ShapeDtypeStruct((rows, 2 * hidden, length), BF16)
    left_call = pl.pallas_call(
        functools.partial(left_kernel, owners, hpo),
        grid=grid,
        in_specs=[smem(), by_rows(pair_act, step), by_rows(pair_mask, step), whole(proj_weight), whole(gate_weight), by_rows(dense, step)]
        + [by_rows(piece, step)] * owners,
        out_specs=[by_rows(part_shape, step), by_rows(dense, step), whole(proj_shape)],
        out_shape=[part_shape, dense, proj_shape],
        scratch_shapes=[turned, pltpu.VMEM((2 * hidden, width), BF16), pltpu.VMEM((2 * hidden, width), F32)],
        compiler_params=params(),
        cost_estimate=cost(12 * count * width * hidden, 12 * count * width),
        name="left",
    )
    part, normed, left_term = left_call(slot, pair_act, pair_mask, proj_weight, gate_weight, d_log, *[da_got[s] for s in range(owners)])
    early = over_chip(
        jnp.concatenate([gate_term, out_term.reshape(hidden, width), left_term.reshape(2 * hidden, width)], axis=0)
    )
    early_sum = over_rest(early)

    right_call = pl.pallas_call(
        functools.partial(right_kernel, owners, hpo),
        grid=grid,
        in_specs=[smem(), by_rows(dense, step), by_rows(pair_mask, step), whole(proj_weight), any_spec]
        + [by_rows(piece, step)] * (2 * owners),
        out_specs=[by_rows(dproj_shape, step), whole(proj_shape)],
        out_shape=[dproj_shape, proj_shape],
        scratch_shapes=[turned, pltpu.VMEM((2 * hidden, width), BF16), pltpu.VMEM((2 * hidden, width), F32)],
        compiler_params=params(),
        cost_estimate=cost(12 * count * width * hidden, 12 * count * width),
        name="right",
    )
    d_proj, right_term = right_call(
        slot, normed, pair_mask, proj_weight, early,
        *[db_got[s] for s in range(owners)],
        *[db_got[s + owners] for s in range(owners)],
    )
    pair_grad = pl.pallas_call(
        finish_kernel,
        grid=grid,
        in_specs=[smem(), by_rows(pair_act, step), whole(proj_weight), by_rows(part_shape, step), by_rows(dproj_shape, step)],
        out_specs=by_rows(dense, step),
        out_shape=dense,
        scratch_shapes=[turned, pltpu.VMEM((2 * hidden, width), BF16)],
        compiler_params=params(),
        cost_estimate=cost(12 * count * width * hidden, 12 * count * width),
        name="finish",
    )(slot, pair_act, proj_weight, part, d_proj)

    right_sum = over_rest(over_chip(right_term.reshape(2 * hidden, width)))
    mine = jnp.concatenate([early_sum, right_sum], axis=0) * (1.0 / length)
    other = send(mine, 1)
    first, second = jnp.where(low, mine, other), jnp.where(low, other, mine)
    n = early_sum.shape[0]
    small = jnp.concatenate([first[:n], second[:n]], axis=0)
    left_sum, right_sum = small[width + hidden :], jnp.concatenate([first[n:], second[n:]], axis=0)
    both = jnp.stack([left_sum.reshape(2, hidden, width), right_sum.reshape(2, hidden, width)], axis=1)
    return (pair_grad, both.reshape(4 * hidden, width).T, small[:width], small[width : width + hidden])


def takes_fast(devices, pair_act, out_weight):
    rows, length, width = pair_act.shape
    hidden = out_weight.shape[0]
    owners = devices // 2
    return (
        devices & (devices - 1) == 0
        and 2 <= devices <= 16
        and rows % 8 == 0
        and hidden == 8 * owners
        and length % 128 == 0
        and width % 128 == 0
        and (owners * rows) % 32 == 0
    )


def normalize_axis(values, axis):
    center = values - jnp.mean(values, axis=axis, keepdims=True)
    scale = lax.rsqrt(jnp.mean(center * center, axis=axis, keepdims=True) + EPS)
    return (center * scale, scale)


def norm_backward(grad, normed, scale, axis):
    first = jnp.mean(grad, axis=axis, keepdims=True)
    second = jnp.mean(grad * normed, axis=axis, keepdims=True)
    return scale * (grad - first - normed * second)


def generic_local(
    pair_act, pair_mask, chain_ids, proj_weight, gate_weight, chain_bias, out_weight, out_grad
):
    devices = lax.axis_size("cells")
    rows_here = pair_act.shape[0]
    length = pair_act.shape[1]
    width = pair_act.shape[2]
    hidden = out_weight.shape[0]
    halfway = length // 2
    channel_pairs = devices // 2
    per_device = 2 * hidden // devices
    count = rows_here * length
    zfull = pair_act.astype(jnp.float32).reshape(count, width)
    zhat, zscale = normalize_axis(zfull, 1)
    normed = zhat.astype(jnp.bfloat16)
    projected = jnp.einsum("xc,cf->fx", normed, proj_weight, preferred_element_type=jnp.float32)
    keeper = pair_mask.astype(jnp.float32).reshape(1, count)
    values = projected[: 2 * hidden]
    sigma = jax.nn.sigmoid(projected[2 * hidden :])
    factors = (keeper * sigma * values).astype(jnp.bfloat16)
    outgoing = factors.reshape(2, channel_pairs, per_device, rows_here, 2, halfway)
    outgoing = jnp.transpose(outgoing, (1, 4, 0, 2, 3, 5)).reshape(
        devices, 2, per_device, rows_here, halfway
    )
    arrived = lax.all_to_all(outgoing, "cells", split_axis=0, concat_axis=3, tiled=True)
    left_half = arrived[0, 0]
    right_half = arrived[0, 1]
    partial_value = jnp.einsum(
        "cik,cjk->cij", left_half, right_half, preferred_element_type=jnp.float32
    )
    landed = lax.all_to_all(
        partial_value.reshape(per_device, devices, rows_here, length).astype(jnp.bfloat16),
        "cells",
        split_axis=1,
        concat_axis=0,
        tiled=True,
    ).astype(jnp.float32)
    landed = landed.reshape(channel_pairs, 2, per_device, rows_here, length)
    triangle = jnp.sum(landed, axis=1).reshape(hidden, count)
    tri_hat, tri_scale = normalize_axis(triangle, 0)
    tri_low = tri_hat.astype(jnp.bfloat16)
    outputs = jnp.einsum("hx,hc->xc", tri_low, out_weight, preferred_element_type=jnp.float32)
    start = lax.axis_index("cells") * rows_here
    own_chain = lax.dynamic_slice_in_dim(chain_ids, start, rows_here, 0)
    same_chain = (own_chain[:, None] == chain_ids[None, :]).reshape(count, 1)
    logits = jnp.dot(normed, gate_weight, preferred_element_type=jnp.float32)
    logits = logits + jnp.where(same_chain, chain_bias[0][None, :], chain_bias[1][None, :])
    gating = jax.nn.sigmoid(logits)
    upstream = out_grad.reshape(count, width).astype(jnp.float32)
    d_outputs = (upstream * gating).astype(jnp.bfloat16)
    d_logits = (upstream * outputs * gating * (1.0 - gating)).astype(jnp.bfloat16)
    out_term = jnp.einsum("hx,xc->hc", tri_low, d_outputs, preferred_element_type=jnp.float32)
    gate_term = jnp.einsum("xc,xd->cd", normed, d_logits, preferred_element_type=jnp.float32)
    d_hat = jnp.einsum("xc,hc->hx", d_outputs, out_weight, preferred_element_type=jnp.float32)
    d_tri = norm_backward(d_hat, tri_hat, tri_scale, 0).astype(jnp.bfloat16)
    doubled = jnp.broadcast_to(
        d_tri.reshape(channel_pairs, 1, per_device, rows_here, length),
        (channel_pairs, 2, per_device, rows_here, length),
    )
    whole = lax.all_to_all(
        doubled.reshape(devices, per_device, rows_here, length),
        "cells",
        split_axis=0,
        concat_axis=2,
        tiled=True,
    )[0]
    d_left = jnp.einsum("cij,cjk->cik", whole, right_half, preferred_element_type=jnp.float32)
    d_right = jnp.einsum("cij,cik->cjk", whole, left_half, preferred_element_type=jnp.float32)
    d_pair = jnp.stack([d_left, d_right]).astype(jnp.bfloat16)
    returned = lax.all_to_all(
        d_pair.reshape(2, per_device, devices, rows_here, halfway),
        "cells",
        split_axis=2,
        concat_axis=2,
        tiled=True,
    )
    returned = returned.reshape(2, per_device, channel_pairs, 2, rows_here, halfway)
    d_factors = (
        jnp.transpose(returned, (0, 2, 1, 4, 3, 5)).reshape(2 * hidden, count).astype(jnp.float32)
    )
    d_values = d_factors * keeper * sigma
    d_gates = d_factors * keeper * values * sigma * (1.0 - sigma)
    d_proj = jnp.concatenate([d_values, d_gates], axis=0).astype(jnp.bfloat16)
    proj_term = jnp.einsum("xc,fx->cf", normed, d_proj, preferred_element_type=jnp.float32)
    d_normed = jnp.einsum("fx,cf->xc", d_proj, proj_weight, preferred_element_type=jnp.float32)
    d_normed = d_normed + jnp.einsum(
        "xd,cd->xc", d_logits, gate_weight, preferred_element_type=jnp.float32
    )
    pair_grad = (
        norm_backward(d_normed, zhat, zscale, 1)
        .astype(jnp.bfloat16)
        .reshape(rows_here, length, width)
    )
    proj_sum, gate_sum, out_sum = lax.psum((proj_term, gate_term, out_term), "cells")
    factor = 1.0 / length
    return (pair_grad, proj_sum * factor, gate_sum * factor, out_sum * factor)


def local(*arrays):
    if takes_fast(lax.axis_size("cells"), arrays[0], arrays[6]):
        return fast_local(*arrays)
    return generic_local(*arrays)


def solution(mesh):
    placed = (
        P(("groups", "cells"), None, None),
        P(("groups", "cells"), None),
        P("groups"),
        P(),
        P(),
        P(),
        P(),
        P(("groups", "cells"), None, None),
    )
    return jax.shard_map(
        local,
        mesh=mesh,
        in_specs=placed,
        out_specs=(
            P(("groups", "cells"), None, None),
            P("groups", None),
            P("groups", None),
            P("groups", None),
        ),
        check_vma=False,
    )
```

```python
import functools

import jax
import jax.numpy as jnp
from jax import lax
from jax.experimental import pallas as pl
from jax.experimental.pallas import tpu as pltpu
from jax.sharding import PartitionSpec as P


EPS = 1e-05
F32 = jnp.float32
BF16 = jnp.bfloat16
MIB = 1024 * 1024

NN = (((1,), (0,)), ((), ()))
NT = (((1,), (1,)), ((), ()))
TN = (((0,), (0,)), ((), ()))


def dot(left, right, dims):
    return lax.dot_general(left, right, dims, preferred_element_type=F32)


def sigmoid(x):
    return 0.5 * jnp.tanh(0.5 * x) + 0.5


def layer_norm(x, axis):
    center = x - jnp.mean(x, axis=axis, keepdims=True)
    scale = lax.rsqrt(jnp.mean(center * center, axis=axis, keepdims=True) + EPS)
    return center * scale, scale


def lane_mean(*terms):
    both = jnp.concatenate(terms, axis=1)
    return dot(both, jnp.full((both.shape[1], terms[0].shape[1]), 1.0 / terms[0].shape[1], BF16), NN)


def row_norm(low):
    return layer_norm(low.astype(F32), 1)


def row_norm_back(grad, normed, scale):
    first = lane_mean(grad.astype(BF16))
    second = lane_mean((grad * normed).astype(BF16))
    return scale * (grad - first - normed * second)


def norm_back(grad, normed, scale, axis):
    first = jnp.mean(grad, axis=axis, keepdims=True)
    second = jnp.mean(grad * normed, axis=axis, keepdims=True)
    return scale * (grad - first - normed * second)


def load_weights(me_ref, proj_ref, t_s, w_s, kinds):
    t_s[...] = proj_ref[...].astype(F32).T.reshape(t_s.shape)
    owners = t_s.shape[0] // 4
    rows = []
    for kind in kinds:
        for s in range(owners):
            block = t_s[kind * owners + (me_ref[0] ^ s)]
            rows.append(block if kind < 2 else 0.5 * block)
    w_s[...] = jnp.concatenate(rows, axis=0).astype(BF16)


def front_kernel(owners, hpo, me_ref, x_ref, mask_ref, wt_ref, *refs):
    zlow_ref, a_ref, b_refs, pairs, (t_s, w_s) = refs[0], refs[1], refs[2 : owners + 2], refs[owners + 2 : -2], refs[-2:]

    @pl.when(pl.program_id(0) == 0)
    def _():
        load_weights(me_ref, wt_ref, t_s, w_s, (0, 1, 2, 3))

    hidden2 = 2 * owners * hpo
    for r in range(x_ref.shape[0]):
        zlow = row_norm(x_ref[r])[0].astype(BF16)
        zlow_ref[r] = zlow
        projected = dot(w_s[...], zlow, NT)
        keep = 0.5 * mask_ref[r : r + 1, :].astype(F32)
        factors = ((keep * jnp.tanh(projected[hidden2:]) + keep) * projected[:hidden2]).astype(BF16)
        for s in range(owners):
            left, right = factors[s * hpo : (s + 1) * hpo], factors[(owners + s) * hpo : (owners + s + 1) * hpo]
            b_refs[s][r] = right
            if s == 0:
                a_ref[r] = left
            else:
                pairs[s - 1][0, r] = left
                pairs[s - 1][1, r] = right


def gate_of(zlow, gw_ref, bias_ref, ids_ref, own):
    logits = dot(zlow, gw_ref[...], NN)
    same = ids_ref[...] == own
    return sigmoid(logits + jnp.where(same, bias_ref[0:1, :], bias_ref[1:2, :]))


def gate_kernel(rows_block, me_ref, own_ref, zlow_ref, up_ref, gw_ref, bias_ref, ids_ref, ow_ref, dout_ref, dhat_ref, w_s):
    step = pl.program_id(0)

    @pl.when(step == 0)
    def _():
        load_ow(me_ref, ow_ref, w_s)

    for r in range(rows_block):
        gating = gate_of(zlow_ref[r], gw_ref, bias_ref, ids_ref, own_ref[step * rows_block + r])
        d_out = (up_ref[r].astype(F32) * gating).astype(BF16)
        dout_ref[r] = d_out
        dhat_ref[r] = dot(w_s[...], d_out, NT)


def load_ow(me_ref, ow_ref, w_s):
    owners = ow_ref.shape[0]
    w_s[...] = jnp.concatenate([ow_ref[me_ref[0] ^ s] for s in range(owners)], axis=0).astype(BF16)


def mid_kernel(owners, hpo, *refs):
    tri, dhat_ref, outs = refs[:owners], refs[owners], refs[owners + 1 :]
    for r in range(dhat_ref.shape[0]):
        triangle = jnp.concatenate([t[r].astype(F32) for t in tri], axis=0)
        tri_hat, scale = layer_norm(triangle, 0)
        d_tri = norm_back(dhat_ref[r], tri_hat, scale, 0).astype(BF16)
        for s in range(owners):
            outs[s][r] = d_tri[s * hpo : (s + 1) * hpo]


def logit_kernel(owners, hpo, rows_block, me_ref, own_ref, zlow_ref, up_ref, dout_ref, gw_ref, bias_ref, ids_ref, ow_ref, *refs):
    tri = refs[:owners]
    dlog_ref, gate_ref, out_ref, w_s, gacc, oacc = refs[owners:]
    step = pl.program_id(0)

    @pl.when(step == 0)
    def _():
        load_ow(me_ref, ow_ref, w_s)
        gacc[...] = jnp.zeros_like(gacc)
        oacc[...] = jnp.zeros_like(oacc)

    for r in range(rows_block):
        zlow = zlow_ref[r]
        gating = gate_of(zlow, gw_ref, bias_ref, ids_ref, own_ref[step * rows_block + r])
        triangle = jnp.concatenate([t[r].astype(F32) for t in tri], axis=0)
        tri_low = layer_norm(triangle, 0)[0].astype(BF16)
        outputs = dot(tri_low, w_s[...], TN)
        d_log = (up_ref[r].astype(F32) * outputs * gating * (1.0 - gating)).astype(BF16)
        dlog_ref[r] = d_log
        oacc[...] += dot(tri_low, dout_ref[r], NN)
        gacc[...] += dot(zlow, d_log, TN)

    @pl.when(step == pl.num_programs(0) - 1)
    def _():
        gate_ref[...] = gacc[...]
        for s in range(owners):
            out_ref[me_ref[0] ^ s] = oacc[s * hpo : (s + 1) * hpo, :]


def part_grad(hidden, mask_row, w_s, zlow, d_fac):
    projected = dot(w_s[...], zlow, NT)
    values, bent = projected[:hidden], jnp.tanh(projected[hidden:])
    keep = 0.5 * mask_row.astype(F32)
    d_values = d_fac * (keep * bent + keep)
    return jnp.concatenate([d_values, d_values * (values - values * bent)], axis=0).astype(BF16)


def store_proj(me_ref, acc, proj_ref, owners, hpo):
    for kind in range(2):
        for s in range(owners):
            start = (kind * owners + s) * hpo
            block = acc[start : start + hpo, :]
            proj_ref[kind, me_ref[0] ^ s] = 0.5 * block if kind else block


def left_kernel(owners, hpo, me_ref, zlow_ref, mask_ref, wt_ref, gw_ref, dlog_ref, *refs):
    da = refs[:owners]
    part_ref, proj_ref, t_s, w_s, acc = refs[owners:]
    step = pl.program_id(0)

    @pl.when(step == 0)
    def _():
        load_weights(me_ref, wt_ref, t_s, w_s, (0, 2))
        acc[...] = jnp.zeros_like(acc)

    for r in range(zlow_ref.shape[0]):
        zlow = zlow_ref[r]
        d_fac = jnp.concatenate([t[r].astype(F32) for t in da], axis=0)
        d_proj = part_grad(owners * hpo, mask_ref[r : r + 1, :], w_s, zlow, d_fac)
        acc[...] += dot(d_proj, zlow, NN)
        part_ref[r] = dot(d_proj, w_s[...], TN) + dot(dlog_ref[r], gw_ref[...], NT)

    @pl.when(step == pl.num_programs(0) - 1)
    def _():
        store_proj(me_ref, acc, proj_ref, owners, hpo)


def right_kernel(owners, hpo, me_ref, zlow_ref, mask_ref, wt_ref, *refs):
    db, dc = refs[:owners], refs[owners : 2 * owners]
    dproj_ref, proj_ref, t_s, w_s, acc = refs[2 * owners :]
    step = pl.program_id(0)

    @pl.when(step == 0)
    def _():
        load_weights(me_ref, wt_ref, t_s, w_s, (1, 3))
        acc[...] = jnp.zeros_like(acc)

    for r in range(zlow_ref.shape[0]):
        zlow = zlow_ref[r]
        d_fac = jnp.concatenate([t[r].astype(F32) + u[r].astype(F32) for t, u in zip(db, dc)], axis=0)
        d_proj = part_grad(owners * hpo, mask_ref[r : r + 1, :], w_s, zlow, d_fac)
        dproj_ref[r] = d_proj
        acc[...] += dot(d_proj, zlow, NN)

    @pl.when(step == pl.num_programs(0) - 1)
    def _():
        store_proj(me_ref, acc, proj_ref, owners, hpo)


def finish_kernel(me_ref, x_ref, wt_ref, part_ref, dproj_ref, *refs):
    pg_ref, t_s, w_s = refs[-3:]

    @pl.when(pl.program_id(0) == 0)
    def _():
        load_weights(me_ref, wt_ref, t_s, w_s, (1, 3))

    for r in range(x_ref.shape[0]):
        zhat, scale = row_norm(x_ref[r])
        d_normed = part_ref[r] + dot(dproj_ref[r], w_s[...], TN)
        pg_ref[r] = row_norm_back(d_normed, zhat, scale).astype(BF16)


def weight_kernel(hidden, scale, core_ref, mine_ref, other_ref, proj_ref, gate_ref, out_ref):
    low = core_ref[0] == 0
    mine, other = mine_ref[...] * scale, other_ref[...] * scale
    first, second = jnp.where(low, mine, other), jnp.where(low, other, mine)
    width = gate_ref.shape[0]
    n = (width + hidden) // 2
    small = jnp.concatenate([first[:n], second[:n]], axis=0)
    gate_ref[...] = small[:width]
    out_ref[...] = small[width:]
    left, right = first[n:], second[n:]
    proj_ref[...] = jnp.concatenate([left[:hidden], right[:hidden], left[hidden:], right[hidden:]], axis=0).T


def shuffle_matrix(rows, hpo):
    n = rows * hpo
    to, frm = lax.broadcasted_iota(jnp.int32, (n, n), 0), lax.broadcasted_iota(jnp.int32, (n, n), 1)
    return jnp.where((to % rows == frm // hpo) & (to // rows == frm % hpo), 1.0, 0.0).astype(BF16)


def spread(p_ref, raw, dest, hpo, group):
    n = group * hpo
    for g in range(raw.shape[0] // n):
        moved = dot(p_ref[...], raw[g * n : (g + 1) * n, :], NN).astype(BF16)
        for h in range(hpo):
            dest[h, g * group : (g + 1) * group, :] = moved[h * group : (h + 1) * group]


def unspread(sums, outs, rows):
    for s in range(len(outs)):
        block = sums[s * rows : (s + 1) * rows]
        outs[s][...] = block.reshape(outs[s].shape).astype(BF16)


def tri_kernel(owners, hpo, rows, group, me_ref, *refs):
    devices = 2 * owners
    pairs = refs[2 : owners + 1]
    a_in = [refs[0]] + [p.at[0] for p in pairs]
    b_in = [refs[1]] + [p.at[1] for p in pairs] + list(refs[owners + 1 : devices + 1])
    refs = refs[devices + 1 :]
    tri_out, a_out, b_out = refs[:owners], refs[owners], refs[owners + 1]
    araw, braw, a_s, b_s, t_s, p_s, sem_a, sem_b, sem_o = refs[owners + 2 :]
    size = rows * hpo
    copies_a = [pltpu.make_async_copy(a_in[s], araw.at[pl.ds(s * size, size)], sem_a.at[s]) for s in range(owners)]
    copies_b = [
        pltpu.make_async_copy(b_in[s], braw.at[pl.ds(pl.multiple_of((me_ref[0] ^ s) * size, size), size)], sem_b.at[s])
        for s in range(devices)
    ]
    for copy in copies_a + copies_b:
        copy.start()
    p_s[...] = shuffle_matrix(group, hpo)
    for copy in copies_a:
        copy.wait()
    spread(p_s, araw, a_s, hpo, group)
    out_a = pltpu.make_async_copy(a_s, a_out, sem_o.at[0])
    out_a.start()
    for copy in copies_b:
        copy.wait()
    spread(p_s, braw, b_s, hpo, group)
    out_b = pltpu.make_async_copy(b_s, b_out, sem_o.at[1])
    out_b.start()
    for h in range(hpo):
        t_s[:, h, :] = dot(a_s[h], b_s[h], NT)
    unspread(t_s, tri_out, rows)
    out_a.wait()
    out_b.wait()


def back_kernel(owners, hpo, rows, group, me_ref, *refs):
    devices = 2 * owners
    d_in, a_in, b_in = refs[:owners], refs[owners], refs[owners + 1]
    refs = refs[owners + 2 :]
    pairs, far_out = refs[2 : owners + 1], refs[owners + 1 : devices + 1]
    da_out = [refs[0]] + [p.at[0] for p in pairs]
    db_out = [refs[1]] + [p.at[1] for p in pairs] + list(far_out)
    draw, d_s, db_s, da_s, t_s, p_s, acc, sem_d, sem_o, sem_a = refs[devices + 1 :]
    size = rows * hpo
    copies = [pltpu.make_async_copy(d_in[s], draw.at[pl.ds(s * size, size)], sem_d.at[s]) for s in range(owners)]
    for copy in copies:
        copy.start()
    p_s[...] = shuffle_matrix(group, hpo)
    for copy in copies:
        copy.wait()
    spread(p_s, draw, d_s, hpo, group)
    for h in range(hpo):
        acc[:, h, :] = dot(d_s[h], a_in[h], TN)
    for s in range(devices):
        db_s[s * size : (s + 1) * size, :] = acc[s * rows : (s + 1) * rows].reshape(size, acc.shape[2]).astype(BF16)
    copies = [
        pltpu.make_async_copy(db_s.at[pl.ds(pl.multiple_of((me_ref[0] ^ s) * size, size), size)], db_out[s], sem_o.at[s])
        for s in range(devices)
    ]
    for copy in copies:
        copy.start()
    for h in range(hpo):
        t_s[:, h, :] = dot(d_s[h], b_in[h], NN)
    da_s[...] = t_s[...].reshape(da_s.shape).astype(BF16)
    copies_a = [pltpu.make_async_copy(da_s.at[pl.ds(s * size, size)], da_out[s], sem_a.at[s]) for s in range(owners)]
    for copy in copies_a:
        copy.start()
    for copy in copies + copies_a:
        copy.wait()


def smem():
    return pl.BlockSpec(memory_space=pltpu.SMEM)


def far(array):
    return pltpu.with_memory_space_constraint(array, pltpu.HBM)


def whole(array):
    return pl.BlockSpec(array.shape, lambda i: (0,) * array.ndim)


def by_rows(array, block):
    return pl.BlockSpec((block,) + array.shape[1:], lambda i: (i,) + (0,) * (array.ndim - 1))


def cost(flops, moved):
    return pl.CostEstimate(flops=flops, bytes_accessed=moved, transcendentals=0)


def params(mib):
    return pltpu.CompilerParams(vmem_limit_bytes=mib * MIB)


def fast_local(pair_act, pair_mask, chain_ids, proj_weight, gate_weight, chain_bias, out_weight, out_grad):
    devices = lax.axis_size("cells")
    owners = devices // 2
    rows, length, width = pair_act.shape
    hidden = out_weight.shape[0]
    hpo = hidden // owners
    count = rows * length
    index = lax.axis_index("cells").astype(jnp.int32)
    me = jnp.reshape(index, (1,))
    slot = jnp.reshape(index % owners, (1,))
    step = 8
    grid = (rows // step,)
    ow = out_weight.astype(F32).reshape(owners, hpo, width)
    turned = pltpu.VMEM((4 * owners, hpo, width), F32)
    piece = jax.ShapeDtypeStruct((rows, hpo, length), BF16)
    flat = jax.ShapeDtypeStruct((rows * hpo, length), BF16)

    def send(array, s):
        return lax.ppermute(array, "cells", [(c, c ^ s) for c in range(devices)])

    both = jax.ShapeDtypeStruct((2,) + piece.shape, BF16)
    both_flat = (2,) + flat.shape
    both_spec = pl.BlockSpec((2, step) + piece.shape[1:], lambda i: (0, i, 0, 0))

    def pick(kind):
        return pl.BlockSpec((None, step) + piece.shape[1:], lambda i: (kind, i, 0, 0))

    normed, *factors = pl.pallas_call(
        functools.partial(front_kernel, owners, hpo),
        grid=grid,
        in_specs=[smem(), by_rows(pair_act, step), by_rows(pair_mask, step), whole(proj_weight)],
        out_specs=[by_rows(pair_act, step)] + [by_rows(piece, step)] * (owners + 1) + [both_spec] * (owners - 1),
        out_shape=[pltpu.HBM(pair_act.shape, BF16)] + [piece] * (owners + 1) + [both] * (owners - 1),
        scratch_shapes=[turned, pltpu.VMEM((4 * hidden, width), BF16)],
        compiler_params=params(12),
        cost_estimate=cost(8 * count * width * hidden, 8 * count * width),
        name="front",
    )(slot, far(pair_act), far(pair_mask), far(proj_weight))
    a_own, b_own, pair_own = factors[0], factors[1 : owners + 1], [None] + factors[owners + 1 :]
    b_far, pair_got = [], [None] * owners
    for s in range(owners, devices):
        b_far.append(send(b_own[s - owners], s))
    for s in range(1, owners):
        pair_got[s] = send(pair_own[s], s)

    start = index * rows
    own_chain = lax.dynamic_slice_in_dim(chain_ids, start, rows, 0)
    ids = jnp.broadcast_to(chain_ids[:, None], (length, width))
    dense = jax.ShapeDtypeStruct((rows, length, width), BF16)
    dhat_shape = jax.ShapeDtypeStruct((rows, hidden, length), F32)
    d_out, d_hat = pl.pallas_call(
        functools.partial(gate_kernel, step),
        grid=grid,
        in_specs=[smem(), smem(), by_rows(pair_act, step), by_rows(out_grad, step), whole(gate_weight), whole(chain_bias), whole(ids), whole(ow)],
        out_specs=[by_rows(dense, step), by_rows(dhat_shape, step)],
        out_shape=[pltpu.HBM(dense.shape, dense.dtype), dhat_shape],
        scratch_shapes=[pltpu.VMEM((hidden, width), BF16)],
        compiler_params=params(16),
        cost_estimate=cost(4 * count * width * width, 12 * count * width),
        name="gate",
    )(slot, own_chain, far(normed), far(out_grad), gate_weight, chain_bias, ids, ow)

    group = 256 // hpo
    half = owners * rows
    any_spec = pl.BlockSpec(memory_space=pl.ANY)
    vmem_spec = pl.BlockSpec(memory_space=pltpu.VMEM)
    tri_results = pl.pallas_call(
        functools.partial(tri_kernel, owners, hpo, rows, group),
        in_specs=[smem()] + [any_spec] * (devices + 1),
        out_specs=[vmem_spec] * owners + [pl.BlockSpec(memory_space=pltpu.HBM)] * 2,
        out_shape=[flat] * owners
        + [pltpu.HBM((hpo, half, length), BF16), pltpu.HBM((hpo, length, length), BF16)],
        scratch_shapes=[
            pltpu.VMEM((half * hpo, length), BF16),
            pltpu.VMEM((length * hpo, length), BF16),
            pltpu.VMEM((hpo, half, length), BF16),
            pltpu.VMEM((hpo, length, length), BF16),
            pltpu.VMEM((half, hpo, length), F32),
            pltpu.VMEM((group * hpo, group * hpo), BF16),
            pltpu.SemaphoreType.DMA((owners,)),
            pltpu.SemaphoreType.DMA((devices,)),
            pltpu.SemaphoreType.DMA((2,)),
        ],
        compiler_params=params(18),
        cost_estimate=cost(2 * hpo * half * length * length, 0),
        name="triangle",
    )(
        me, a_own.reshape(flat.shape), b_own[0].reshape(flat.shape),
        *[pair_got[s].reshape(both_flat) for s in range(1, owners)],
        *[b.reshape(flat.shape) for b in b_far],
    )
    tri_own, a_all, b_all = tri_results[:owners], tri_results[owners], tri_results[owners + 1]
    tri_got = {0: tri_own[0].reshape(piece.shape)}
    for s in range(owners - 1, 0, -1):
        tri_got[s] = send(tri_own[s].reshape(piece.shape), s)
    tri = [tri_got[s] for s in range(owners)]

    d_own = pl.pallas_call(
        functools.partial(mid_kernel, owners, hpo),
        grid=grid,
        in_specs=[by_rows(piece, step)] * owners + [by_rows(dhat_shape, step)],
        out_specs=[by_rows(piece, step)] * owners,
        out_shape=[piece] * owners,
        compiler_params=params(10),
        cost_estimate=cost(20 * count * hidden, 8 * count * hidden),
        name="middle",
    )(*tri, d_hat)
    d_got = {0: d_own[0]}
    for s in range(owners - 1, 0, -1):
        d_got[s] = send(d_own[s], s)

    gate_shape = jax.ShapeDtypeStruct((width, width), F32)
    out_shape = jax.ShapeDtypeStruct((owners, hpo, width), F32)
    d_log, gate_term, out_term = pl.pallas_call(
        functools.partial(logit_kernel, owners, hpo, step),
        grid=grid,
        in_specs=[smem(), smem(), by_rows(pair_act, step), by_rows(out_grad, step), by_rows(dense, step), whole(gate_weight), whole(chain_bias), whole(ids), whole(ow)]
        + [by_rows(piece, step)] * owners,
        out_specs=[by_rows(dense, step), whole(gate_shape), whole(out_shape)],
        out_shape=[pltpu.HBM(dense.shape, dense.dtype), gate_shape, out_shape],
        scratch_shapes=[pltpu.VMEM((hidden, width), BF16), pltpu.VMEM((width, width), F32), pltpu.VMEM((hidden, width), F32)],
        compiler_params=params(16),
        cost_estimate=cost(8 * count * width * width, 10 * count * width),
        name="logits",
    )(slot, own_chain, far(normed), far(out_grad), far(d_out), gate_weight, chain_bias, ids, ow, *tri)

    low = index % 2 == 0

    def over_chip(term):
        n = term.shape[0] // 2
        first, second = term[:n], term[n:]
        mine = jnp.where(low, first, second) + send(jnp.where(low, second, first), 1)
        return mine + send(mine, 2)

    def over_rest(term):
        return term + sum(send(term, s) for s in range(4, devices, 4))

    early_sum = over_rest(over_chip(jnp.concatenate([gate_term, out_term.reshape(hidden, width)], axis=0)))

    back_call = pl.pallas_call(
        functools.partial(back_kernel, owners, hpo, rows, group),
        in_specs=[smem()] + [any_spec] * owners + [vmem_spec] * 2,
        out_specs=[pl.BlockSpec(memory_space=pltpu.HBM)] * (devices + 1),
        out_shape=[pltpu.HBM(flat.shape, BF16)] * 2
        + [pltpu.HBM(both_flat, BF16)] * (owners - 1)
        + [pltpu.HBM(flat.shape, BF16)] * owners,
        scratch_shapes=[
            pltpu.VMEM((half * hpo, length), BF16),
            pltpu.VMEM((hpo, half, length), BF16),
            pltpu.VMEM((length * hpo, length), BF16),
            pltpu.VMEM((half * hpo, length), BF16),
            pltpu.VMEM((half, hpo, length), F32),
            pltpu.VMEM((group * hpo, group * hpo), BF16),
            pltpu.VMEM((length, hpo, length), F32),
            pltpu.SemaphoreType.DMA((owners,)),
            pltpu.SemaphoreType.DMA((devices,)),
            pltpu.SemaphoreType.DMA((owners,)),
        ],
        compiler_params=params(22),
        cost_estimate=cost(4 * hpo * half * length * length, 0),
        name="back",
    )
    back = back_call(me, *[d_got[s].reshape(flat.shape) for s in range(owners)], a_all, b_all)
    da_own, db_own = back[0].reshape(piece.shape), back[1].reshape(piece.shape)
    db_far, home = [], []
    for s in range(owners, devices):
        db_far.append(send(back[s + 1].reshape(piece.shape), s))
    for s in range(1, owners):
        home.append(send(back[s + 1].reshape(both.shape), s))

    proj_shape = jax.ShapeDtypeStruct((2, owners, hpo, width), F32)
    part_shape = jax.ShapeDtypeStruct((rows, length, width), F32)
    dproj_shape = jax.ShapeDtypeStruct((rows, 2 * hidden, length), BF16)
    left_call = pl.pallas_call(
        functools.partial(left_kernel, owners, hpo),
        grid=grid,
        in_specs=[smem(), by_rows(pair_act, step), by_rows(pair_mask, step), whole(proj_weight), whole(gate_weight), by_rows(dense, step)]
        + [by_rows(piece, step)] + [pick(0)] * (owners - 1),
        out_specs=[by_rows(part_shape, step), whole(proj_shape)],
        out_shape=[part_shape, proj_shape],
        scratch_shapes=[turned, pltpu.VMEM((2 * hidden, width), BF16), pltpu.VMEM((2 * hidden, width), F32)],
        compiler_params=params(16),
        cost_estimate=cost(12 * count * width * hidden, 12 * count * width),
        name="left",
    )
    part, left_term = left_call(slot, far(normed), pair_mask, proj_weight, gate_weight, far(d_log), da_own, *home)

    right_call = pl.pallas_call(
        functools.partial(right_kernel, owners, hpo),
        grid=grid,
        in_specs=[smem(), by_rows(dense, step), by_rows(pair_mask, step), whole(proj_weight)]
        + [by_rows(piece, step)] + [pick(1)] * (owners - 1) + [by_rows(piece, step)] * owners,
        out_specs=[by_rows(dproj_shape, step), whole(proj_shape)],
        out_shape=[dproj_shape, proj_shape],
        scratch_shapes=[turned, pltpu.VMEM((2 * hidden, width), BF16), pltpu.VMEM((2 * hidden, width), F32)],
        compiler_params=params(14),
        cost_estimate=cost(12 * count * width * hidden, 12 * count * width),
        name="right",
    )
    d_proj, right_term = right_call(
        slot, normed, pair_mask, proj_weight,
        db_own, *home, *db_far,
    )

    def finish(first, blocks, *before):
        def rows_of(array):
            return pl.BlockSpec((step,) + array.shape[1:], lambda i: (i + first,) + (0,) * (len(array.shape) - 1))

        return pl.pallas_call(
            finish_kernel,
            grid=(blocks,),
            in_specs=[smem(), rows_of(pair_act), whole(proj_weight), rows_of(part_shape), rows_of(dproj_shape)] + [any_spec] * len(before),
            out_specs=rows_of(dense),
            out_shape=dense,
            input_output_aliases={5: 0} if before else {},
            scratch_shapes=[turned, pltpu.VMEM((2 * hidden, width), BF16)],
            compiler_params=params(14),
            cost_estimate=cost(4 * blocks * step * length * width * hidden, 4 * blocks * step * length * width),
            name="finish",
        )(slot, pair_act, proj_weight, part, d_proj, *before)

    pair_grad = finish(0, 1)
    pair_grad = finish(1, rows // step - 1, pair_grad) if rows > step else pair_grad
    terms = jnp.concatenate([left_term.reshape(2 * hidden, width), right_term.reshape(2 * hidden, width)], axis=0)
    late_sum = over_rest(over_chip(terms))
    mine = jnp.concatenate([early_sum, late_sum], axis=0)
    other = send(mine, 1)
    proj_sum, gate_sum, out_sum = pl.pallas_call(
        functools.partial(weight_kernel, hidden, 1.0 / length),
        in_specs=[smem()] + [vmem_spec] * 2,
        out_specs=[vmem_spec] * 3,
        out_shape=[jax.ShapeDtypeStruct(proj_weight.shape, F32), gate_shape, jax.ShapeDtypeStruct(out_weight.shape, F32)],
        compiler_params=params(8),
        name="weights",
    )(jnp.reshape(index % 2, (1,)), mine, other)
    return (pair_grad, proj_sum, gate_sum, out_sum)


def takes_fast(devices, pair_act, out_weight):
    rows, length, width = pair_act.shape
    hidden = out_weight.shape[0]
    owners = devices // 2
    return (
        devices & (devices - 1) == 0
        and 2 <= devices <= 16
        and rows % 8 == 0
        and hidden == 8 * owners
        and length % 128 == 0
        and width % 128 == 0
        and (owners * rows) % 32 == 0
    )


def normalize_axis(values, axis):
    center = values - jnp.mean(values, axis=axis, keepdims=True)
    scale = lax.rsqrt(jnp.mean(center * center, axis=axis, keepdims=True) + EPS)
    return (center * scale, scale)


def norm_backward(grad, normed, scale, axis):
    first = jnp.mean(grad, axis=axis, keepdims=True)
    second = jnp.mean(grad * normed, axis=axis, keepdims=True)
    return scale * (grad - first - normed * second)


def generic_local(
    pair_act, pair_mask, chain_ids, proj_weight, gate_weight, chain_bias, out_weight, out_grad
):
    devices = lax.axis_size("cells")
    rows_here = pair_act.shape[0]
    length = pair_act.shape[1]
    width = pair_act.shape[2]
    hidden = out_weight.shape[0]
    halfway = length // 2
    channel_pairs = devices // 2
    per_device = 2 * hidden // devices
    count = rows_here * length
    zfull = pair_act.astype(jnp.float32).reshape(count, width)
    zhat, zscale = normalize_axis(zfull, 1)
    normed = zhat.astype(jnp.bfloat16)
    projected = jnp.einsum("xc,cf->fx", normed, proj_weight, preferred_element_type=jnp.float32)
    keeper = pair_mask.astype(jnp.float32).reshape(1, count)
    values = projected[: 2 * hidden]
    sigma = jax.nn.sigmoid(projected[2 * hidden :])
    factors = (keeper * sigma * values).astype(jnp.bfloat16)
    outgoing = factors.reshape(2, channel_pairs, per_device, rows_here, 2, halfway)
    outgoing = jnp.transpose(outgoing, (1, 4, 0, 2, 3, 5)).reshape(
        devices, 2, per_device, rows_here, halfway
    )
    arrived = lax.all_to_all(outgoing, "cells", split_axis=0, concat_axis=3, tiled=True)
    left_half = arrived[0, 0]
    right_half = arrived[0, 1]
    partial_value = jnp.einsum(
        "cik,cjk->cij", left_half, right_half, preferred_element_type=jnp.float32
    )
    landed = lax.all_to_all(
        partial_value.reshape(per_device, devices, rows_here, length).astype(jnp.bfloat16),
        "cells",
        split_axis=1,
        concat_axis=0,
        tiled=True,
    ).astype(jnp.float32)
    landed = landed.reshape(channel_pairs, 2, per_device, rows_here, length)
    triangle = jnp.sum(landed, axis=1).reshape(hidden, count)
    tri_hat, tri_scale = normalize_axis(triangle, 0)
    tri_low = tri_hat.astype(jnp.bfloat16)
    outputs = jnp.einsum("hx,hc->xc", tri_low, out_weight, preferred_element_type=jnp.float32)
    start = lax.axis_index("cells") * rows_here
    own_chain = lax.dynamic_slice_in_dim(chain_ids, start, rows_here, 0)
    same_chain = (own_chain[:, None] == chain_ids[None, :]).reshape(count, 1)
    logits = jnp.dot(normed, gate_weight, preferred_element_type=jnp.float32)
    logits = logits + jnp.where(same_chain, chain_bias[0][None, :], chain_bias[1][None, :])
    gating = jax.nn.sigmoid(logits)
    upstream = out_grad.reshape(count, width).astype(jnp.float32)
    d_outputs = (upstream * gating).astype(jnp.bfloat16)
    d_logits = (upstream * outputs * gating * (1.0 - gating)).astype(jnp.bfloat16)
    out_term = jnp.einsum("hx,xc->hc", tri_low, d_outputs, preferred_element_type=jnp.float32)
    gate_term = jnp.einsum("xc,xd->cd", normed, d_logits, preferred_element_type=jnp.float32)
    d_hat = jnp.einsum("xc,hc->hx", d_outputs, out_weight, preferred_element_type=jnp.float32)
    d_tri = norm_backward(d_hat, tri_hat, tri_scale, 0).astype(jnp.bfloat16)
    doubled = jnp.broadcast_to(
        d_tri.reshape(channel_pairs, 1, per_device, rows_here, length),
        (channel_pairs, 2, per_device, rows_here, length),
    )
    whole = lax.all_to_all(
        doubled.reshape(devices, per_device, rows_here, length),
        "cells",
        split_axis=0,
        concat_axis=2,
        tiled=True,
    )[0]
    d_left = jnp.einsum("cij,cjk->cik", whole, right_half, preferred_element_type=jnp.float32)
    d_right = jnp.einsum("cij,cik->cjk", whole, left_half, preferred_element_type=jnp.float32)
    d_pair = jnp.stack([d_left, d_right]).astype(jnp.bfloat16)
    returned = lax.all_to_all(
        d_pair.reshape(2, per_device, devices, rows_here, halfway),
        "cells",
        split_axis=2,
        concat_axis=2,
        tiled=True,
    )
    returned = returned.reshape(2, per_device, channel_pairs, 2, rows_here, halfway)
    d_factors = (
        jnp.transpose(returned, (0, 2, 1, 4, 3, 5)).reshape(2 * hidden, count).astype(jnp.float32)
    )
    d_values = d_factors * keeper * sigma
    d_gates = d_factors * keeper * values * sigma * (1.0 - sigma)
    d_proj = jnp.concatenate([d_values, d_gates], axis=0).astype(jnp.bfloat16)
    proj_term = jnp.einsum("xc,fx->cf", normed, d_proj, preferred_element_type=jnp.float32)
    d_normed = jnp.einsum("fx,cf->xc", d_proj, proj_weight, preferred_element_type=jnp.float32)
    d_normed = d_normed + jnp.einsum(
        "xd,cd->xc", d_logits, gate_weight, preferred_element_type=jnp.float32
    )
    pair_grad = (
        norm_backward(d_normed, zhat, zscale, 1)
        .astype(jnp.bfloat16)
        .reshape(rows_here, length, width)
    )
    proj_sum, gate_sum, out_sum = lax.psum((proj_term, gate_term, out_term), "cells")
    factor = 1.0 / length
    return (pair_grad, proj_sum * factor, gate_sum * factor, out_sum * factor)


def local(*arrays):
    if takes_fast(lax.axis_size("cells"), arrays[0], arrays[6]):
        return fast_local(*arrays)
    return generic_local(*arrays)


def solution(mesh):
    placed = (
        P(("groups", "cells"), None, None),
        P(("groups", "cells"), None),
        P("groups"),
        P(),
        P(),
        P(),
        P(),
        P(("groups", "cells"), None, None),
    )
    return jax.shard_map(
        local,
        mesh=mesh,
        in_specs=placed,
        out_specs=(
            P(("groups", "cells"), None, None),
            P("groups", None),
            P("groups", None),
            P("groups", None),
        ),
        check_vma=False,
    )
```
